128 devices in a mesh: frame: 64 (over x, z_lo, y, core), row: 2 (over z_hi).
Axes of the slice: x: 4, y: 4, z: 4 (z_hi: 2, z_lo: 2; z = z_hi * 2 + z_lo), core: 2. Of those that a mesh axis runs over, the one named last changes fastest.
Arguments:
- footage: float32 [256, 1024, 1024], P('frame', 'row'), may hold values from -30 to 30
Outputs:
- coefficients: float32 [256, 1024, 1024], P('frame', 'row')
- energies: float32 [4, 10], replicated
The draws below stay inside these ranges and needn't reach their ends.
All inputs are finite; a program needn't handle non-finite values.
Results may differ from the reference program's by a relative error of at most 0.00007.
Values sent between devices are 32-bit elements; how exact they have to be, the bound alone decides.
A program may use at most 128 MiB of HBM per device.

```python
import math
from functools import partial
import jax
import jax.numpy as jnp
import numpy as np
from jax import lax

H = 1024
W = 1024
SLEVELS = 3
TLEVELS = 3
FRAMES = 256


def draw_footage(key, part):
    subkeys = jax.random.split(jax.random.fold_in(key, 7), 1)
    full_shape = (FRAMES, H, W)
    frame_ramp = jnp.arange(FRAMES, dtype=jnp.float32) / (FRAMES - 1)
    values = jnp.clip(jax.random.normal(subkeys[0], full_shape, jnp.float32), -5.0, 5.0)
    values = values * jnp.exp(math.log(3.0) * frame_ramp)[:, None, None]
    return values


def setup_inputs(seed: int = 0) -> dict:
    keys = jax.random.split(jax.random.key(seed), 2)
    return {
        "footage": draw_footage(jax.random.fold_in(keys[1], 71), 0),
    }


LIFT_ALPHA = -1.586134342
LIFT_BETA = -0.05298011854
LIFT_GAMMA = 0.8829110762
LIFT_DELTA = 0.4435068522
LIFT_ZETA = 1.149604398


def mirror_after(values, along):
    length = values.shape[along]
    return jnp.concatenate([lax.slice_in_dim(values, 1, length, axis=along), lax.slice_in_dim(values, length - 1, length, axis=along)], axis=along)


def mirror_before(values, along):
    length = values.shape[along]
    return jnp.concatenate([lax.slice_in_dim(values, 0, 1, axis=along), lax.slice_in_dim(values, 0, length - 1, axis=along)], axis=along)


def weave_axis(even_part, odd_part, along):
    stacked = jnp.stack([even_part, odd_part], axis=along + 1)
    new_shape = list(even_part.shape)
    new_shape[along] = new_shape[along] * 2
    return stacked.reshape(tuple(new_shape))


def lift_pair(even_part, odd_part, take_next, take_prev):
    odd_part = odd_part + LIFT_ALPHA * (even_part + take_next(even_part))
    even_part = even_part + LIFT_BETA * (take_prev(odd_part) + odd_part)
    odd_part = odd_part + LIFT_GAMMA * (even_part + take_next(even_part))
    even_part = even_part + LIFT_DELTA * (take_prev(odd_part) + odd_part)
    return even_part * LIFT_ZETA, odd_part * (1.0 / LIFT_ZETA)


def spatial(planes_in, levels, take_next, take_prev):
    row_axis = planes_in.ndim - 2
    col_axis = planes_in.ndim - 1
    low_cols, high_cols = lift_pair(planes_in[..., 0::2], planes_in[..., 1::2], partial(mirror_after, along=col_axis), partial(mirror_before, along=col_axis))
    combined = jnp.concatenate([low_cols, high_cols], axis=col_axis)
    low_rows, high_rows = lift_pair(combined[..., 0::2, :], combined[..., 1::2, :], take_next, take_prev)
    half_width = low_cols.shape[-1]
    coarse = low_rows[..., :half_width]
    if levels > 1:
        coarse = spatial(coarse, levels - 1, take_next, take_prev)
    upper_rows = weave_axis(coarse, low_rows[..., half_width:], col_axis)
    bottom = weave_axis(high_rows[..., :half_width], high_rows[..., half_width:], col_axis)
    return weave_axis(upper_rows, bottom, row_axis)


def temporal(planes_in, levels):
    even_part = planes_in[0::2]
    odd_part = planes_in[1::2]
    odd_part = odd_part - 0.5 * (even_part + mirror_after(even_part, 0))
    even_part = even_part + 0.25 * (mirror_before(odd_part, 0) + odd_part)
    if levels > 1:
        even_part = temporal(even_part, levels - 1)
    return weave_axis(even_part, odd_part, 0)


def level_of(number, ceiling):
    depth_now = 1
    while number % 2 == 0 and depth_now <= ceiling:
        number = number // 2
        depth_now = depth_now + 1
    return depth_now


def space_table(levels):
    period = 2 ** levels
    band_table = np.zeros((period * period, 3 * levels + 1), np.float32)
    for row_pos in range(period):
        for col_pos in range(period):
            row_level = level_of(row_pos, levels)
            col_level = level_of(col_pos, levels)
            finest = min(row_level, col_level)
            if finest > levels:
                column = 3 * levels
            elif row_level == col_level:
                column = 3 * (finest - 1) + 2
            elif row_level == finest:
                column = 3 * (finest - 1)
            else:
                column = 3 * (finest - 1) + 1
            band_table[row_pos * period + col_pos, column] = 1.0
    return band_table


def time_table(levels):
    period = 2 ** levels
    band_table = np.zeros((period, levels + 1), np.float32)
    for number in range(period):
        band_table[number, level_of(number, levels) - 1] = 1.0
    return band_table


def band_sums(coeffs, first_frame, levels_s, levels_t):
    period = 2 ** levels_s
    frame_count, row_count, col_count = coeffs.shape
    square = coeffs * coeffs
    pattern = square.reshape(frame_count, row_count // period, period, col_count // period, period).sum(axis=(1, 3))
    pattern = pattern.reshape(frame_count, period * period)
    per_frame = jnp.dot(pattern, jnp.asarray(space_table(levels_s), jnp.float32), precision=lax.Precision.HIGHEST)
    time_period = 2 ** levels_t
    position = (first_frame + jnp.arange(frame_count, dtype=jnp.int32)) % time_period
    onehot = (position[:, None] == jnp.arange(time_period, dtype=jnp.int32)[None, :]).astype(jnp.float32)
    frame_band = jnp.dot(onehot, jnp.asarray(time_table(levels_t), jnp.float32), precision=lax.Precision.HIGHEST)
    return jnp.dot(frame_band.T, per_frame, precision=lax.Precision.HIGHEST)


def band_means(totals, frames_all, rows_all, cols_all, levels_s, levels_t):
    space_share = space_table(levels_s).sum(0) / float((2 ** levels_s) ** 2)
    time_share = time_table(levels_t).sum(0) / float(2 ** levels_t)
    counts = float(frames_all) * float(rows_all) * float(cols_all) * np.outer(time_share, space_share)
    return totals / jnp.asarray(counts, jnp.float32)


def reference(footage):
    frames_all, rows_all, cols_all = footage.shape

    def picture_step(picture):
        return spatial(picture[None], SLEVELS, partial(mirror_after, along=1), partial(mirror_before, along=1))[0]

    planes = lax.map(picture_step, footage)
    block_rows = 8
    grouped = jnp.moveaxis(planes.reshape(frames_all, rows_all // block_rows, block_rows, cols_all), 1, 0)

    def time_step(row_block):
        return temporal(row_block, TLEVELS)

    temporal_out = lax.map(time_step, grouped)
    coeffs = jnp.moveaxis(temporal_out, 0, 1).reshape(frames_all, rows_all, cols_all)
    totals = band_sums(coeffs, 0, SLEVELS, TLEVELS)
    return coeffs, band_means(totals, frames_all, rows_all, cols_all, SLEVELS, TLEVELS)
```

```python
import functools

import jax
import jax.numpy as jnp
import ml_dtypes
import numpy as np
from jax import lax
from jax.experimental import pallas as pl
from jax.experimental.pallas import tpu as pltpu
from jax.sharding import PartitionSpec as P

SLEVELS = 3
TLEVELS = 3
ALPHA = -1.586134342
BETA = -0.05298011854
GAMMA = 0.8829110762
DELTA = 0.4435068522
ZETA = 1.149604398
HALO = 32
PAD = 8
LANES = 128


def lift_matrix(width):
    x = np.eye(width)
    e, o = x[:, 0::2], x[:, 1::2]
    after = lambda v: np.concatenate([v[:, 1:], v[:, -1:]], axis=1)
    before = lambda v: np.concatenate([v[:, :1], v[:, :-1]], axis=1)
    o = o + ALPHA * (e + after(e))
    e = e + BETA * (before(o) + o)
    o = o + GAMMA * (e + after(e))
    e = e + DELTA * (before(o) + o)
    out = np.zeros((width, width))
    out[:, 0::2] = e * ZETA
    out[:, 1::2] = o * (1.0 / ZETA)
    return out


def weight_blocks(width):
    levels = []
    for level in range(SLEVELS):
        s = 2**level
        m = np.zeros((width, width))
        m[::s, ::s] = lift_matrix(width // s)
        b = LANES
        mid = width // 2
        blocks = np.stack([
            m[:b, :b],
            m[mid:mid + b, mid:mid + b],
            m[width - b:, width - b:],
            m[mid - b:mid, mid:mid + b],
            m[mid + b:mid + 2 * b, mid:mid + b],
        ])
        hi = blocks.astype(ml_dtypes.bfloat16)
        lo = (blocks - hi.astype(np.float64)).astype(ml_dtypes.bfloat16)
        levels.append(np.stack([hi, lo]))
    return np.stack(levels)


TILES = (
    ((0, 3), (4, 1), (None, 4), (None, None)),
    ((3, None), (1, 3), (4, 1), (None, 4)),
    ((None, None), (3, None), (1, 3), (4, 2)),
)


def build_weights(blocks_ref, w_ref):
    zero = jnp.zeros((LANES, LANES), jnp.bfloat16)

    def fill(index, carry):
        level, part = index // 2, index % 2
        for kind in range(3):
            for r in range(4):
                for c in range(2):
                    which = TILES[kind][r][c]
                    value = zero if which is None else blocks_ref[level, part, which]
                    w_ref[level, part, kind, r * LANES:(r + 1) * LANES, c * LANES:(c + 1) * LANES] = value
        return carry

    lax.fori_loop(0, SLEVELS * 2, fill, 0)


def columns(xs, w_ref, level, store):
    count = len(xs)
    his, los = [], []
    for x in xs:
        hi = x.astype(jnp.bfloat16)
        his.append(hi)
        los.append((x - hi.astype(jnp.float32)).astype(jnp.bfloat16))
    for tile in range(count // 2):
        if tile == 0:
            kind, start = 0, 0
        elif tile == count // 2 - 1:
            kind, start = 2, count - 4
        else:
            kind, start = 1, 2 * tile - 1
        hi = jnp.concatenate(his[start:start + 4], axis=1)
        lo = jnp.concatenate(los[start:start + 4], axis=1)
        whi = w_ref[level, 0, kind]
        wlo = w_ref[level, 1, kind]
        dot = functools.partial(jnp.dot, preferred_element_type=jnp.float32)
        acc = dot(hi, whi) + dot(lo, whi) + dot(hi, wlo)
        store(2 * tile, acc[:, :LANES])
        store(2 * tile + 1, acc[:, LANES:])


def lift_rows(buf, pairs):
    ev = pl.ds(PAD, pairs, stride=2)
    od = pl.ds(PAD + 1, pairs, stride=2)
    ev_next = pl.ds(PAD + 2, pairs, stride=2)
    od_prev = pl.ds(PAD - 1, pairs, stride=2)
    end = PAD + 2 * pairs

    def panel(p, carry):
        def mirror_end():
            buf[p, end:end + 1, :] = buf[p, end - 2:end - 1, :]

        def mirror_start():
            buf[p, PAD - 1:PAD, :] = buf[p, PAD + 1:PAD + 2, :]

        mirror_end()
        buf[p, od, :] = buf[p, od, :] * (1.0 / ZETA) + (ALPHA / ZETA) * (buf[p, ev, :] + buf[p, ev_next, :])
        mirror_start()
        buf[p, ev, :] = buf[p, ev, :] + (BETA * ZETA) * (buf[p, od_prev, :] + buf[p, od, :])
        mirror_end()
        buf[p, od, :] = buf[p, od, :] + (GAMMA / ZETA) * (buf[p, ev, :] + buf[p, ev_next, :])
        mirror_start()
        buf[p, ev, :] = buf[p, ev, :] * ZETA + (DELTA * ZETA * ZETA) * (buf[p, od_prev, :] + buf[p, od, :])
        return carry

    lax.fori_loop(0, buf.shape[0], panel, 0)


def spatial(own, halo, upper, w_ref, bufs, write):
    one, two, three = bufs
    panels = one.shape[0]
    rows = one.shape[1] - 2 * PAD
    strip = rows - HALO
    own_at = PAD + HALO * upper
    halo_at = PAD + strip * (1 - upper)
    half = strip // 2

    def store_top(p, value):
        one[p, pl.ds(pl.multiple_of(own_at, 8), half), :] = value

    def store_rest(p, value):
        one[p, pl.ds(pl.multiple_of(own_at + half, 8), half), :] = value[:half]
        one[p, pl.ds(pl.multiple_of(halo_at, 8), HALO), :] = value[half:]

    columns(own(0, half), w_ref, 0, store_top)
    rest = [jnp.concatenate(pair, axis=0) for pair in zip(own(half, half), halo())]
    columns(rest, w_ref, 0, store_rest)
    lift_rows(one, rows // 2)

    def into(buf, n):
        def store(p, value):
            buf[p, PAD:PAD + n, :] = value
        return store

    def evens(buf, n):
        return [buf[p, pl.ds(PAD, n, stride=2), :] for p in range(panels)]

    columns(evens(one, rows // 2), w_ref, 1, into(two, rows // 2))
    lift_rows(two, rows // 4)
    columns(evens(two, rows // 4), w_ref, 2, into(three, rows // 4))
    lift_rows(three, rows // 8)

    def merge(p, carry):
        lane = lax.broadcasted_iota(jnp.int32, (1, LANES), 1)
        n = rows // 4
        old = two[p, pl.ds(PAD, n, stride=2), :]
        two[p, pl.ds(PAD, n, stride=2), :] = jnp.where(lane % 4 == 0, three[p, PAD:PAD + n, :], old)
        n = rows // 2
        old = one[p, pl.ds(PAD, n, stride=2), :]
        one[p, pl.ds(PAD, n, stride=2), :] = jnp.where(lane % 2 == 0, two[p, PAD:PAD + n, :], old)
        return carry

    lax.fori_loop(0, panels, merge, 0)
    for p in range(panels):
        write(p, one[p, pl.ds(pl.multiple_of(own_at, 8), strip), :])


def level_of(number, ceiling):
    depth = 1
    while number % 2 == 0 and depth <= ceiling:
        number //= 2
        depth += 1
    return depth


def band_of(row, col):
    u, v = level_of(row, SLEVELS), level_of(col, SLEVELS)
    m = min(u, v)
    if m > SLEVELS:
        return 3 * SLEVELS
    if u == v:
        return 3 * (m - 1) + 2
    return 3 * (m - 1) + (0 if u == m else 1)


def position_level(pos):
    return jnp.where(pos % 2 == 1, 1, jnp.where(pos % 4 == 2, 2, jnp.where(pos % 8 == 4, 3, 4)))


def band_table(shape):
    u = position_level(lax.broadcasted_iota(jnp.int32, shape, 0))
    v = position_level(lax.broadcasted_iota(jnp.int32, shape, 1))
    m = jnp.minimum(u, v)
    kind = jnp.where(u == v, 2, jnp.where(u == m, 0, 1))
    return jnp.where(m == SLEVELS + 1, 3 * SLEVELS, 3 * (m - 1) + kind)


def spatial_kernel(own_ref, halo_ref, blocks_ref, out_ref, energy_ref, w_ref, one, two, three):
    plane = pl.program_id(0)
    upper = lax.axis_index("row")
    core = lax.axis_index("frame") % 2
    panels = one.shape[0]

    @pl.when(plane == 0)
    def _():
        build_weights(blocks_ref, w_ref)
        energy_ref[...] = jnp.zeros_like(energy_ref)

    def own(r, m):
        return [own_ref[0, r:r + m, p * LANES:(p + 1) * LANES] for p in range(panels)]

    def halo():
        return [halo_ref[0, :, p * LANES:(p + 1) * LANES] for p in range(panels)]

    squares = []

    def write(p, value):
        out_ref[0, :, p * LANES:(p + 1) * LANES] = value
        squares.append((value * value).reshape(-1, 8, LANES).sum(axis=0))

    spatial(own, halo, upper, w_ref, (one, two, three), write)
    total = functools.reduce(jnp.add, squares)
    time_band = jnp.where(plane == 0, jnp.where(core == 0, 3, 2), jnp.where(plane == 2, 1, 0))
    bands = band_table((8, LANES))
    row = lax.broadcasted_iota(jnp.int32, (8, LANES), 0)
    col = lax.broadcasted_iota(jnp.int32, (8, LANES), 1)
    acc = energy_ref[...]
    for s in range(3 * SLEVELS + 1):
        part = jnp.sum(jnp.where(bands == s, total, 0.0))
        acc = acc + jnp.where((row == time_band) & (col == s), part, 0.0)
    energy_ref[...] = acc


def spatial_call(planes, halos):
    n, strip, width = planes.shape
    panels = width // LANES
    rows = strip + HALO
    blocks = jnp.asarray(weight_blocks(width))
    scratch = lambda r: pltpu.VMEM((panels, r + 2 * PAD, LANES), jnp.float32)
    return pl.pallas_call(
        spatial_kernel,
        grid=(n,),
        out_shape=(
            jax.ShapeDtypeStruct((n, strip, width), jnp.float32),
            jax.ShapeDtypeStruct((8, LANES), jnp.float32),
        ),
        in_specs=[
            pl.BlockSpec((1, strip, width), lambda i: (i, 0, 0)),
            pl.BlockSpec((1, HALO, width), lambda i: (i, 0, 0)),
            pl.BlockSpec(memory_space=pltpu.VMEM),
        ],
        out_specs=(
            pl.BlockSpec((1, strip, width), lambda i: (i, 0, 0)),
            pl.BlockSpec((8, LANES), lambda i: (0, 0)),
        ),
        scratch_shapes=[
            pltpu.VMEM((SLEVELS, 2, 3, 4 * LANES, 2 * LANES), jnp.bfloat16),
            scratch(rows),
            scratch(rows // 2),
            scratch(rows // 4),
        ],
        compiler_params=pltpu.CompilerParams(vmem_limit_bytes=44 * 2**20),
        name="spatial",
    )(planes, halos, blocks)


def counts(frames, rows, cols):
    table = np.zeros(3 * SLEVELS + 1)
    for i in range(8):
        for j in range(8):
            table[band_of(i, j)] += 1 / 64
    share = np.array([0.5, 0.25, 0.125, 0.125])
    return float(frames) * rows * cols * np.outer(share, table)


def shards(footage):
    me = lax.axis_index("frame")
    devices = lax.axis_size("frame")
    first, last = me == 0, me == devices - 1
    odd = me % 2 == 1
    left = lambda x: lax.ppermute(x, "frame", [(i, i - 1) for i in range(1, devices)])
    right = lambda x: lax.ppermute(x, "frame", [(i, i + 1) for i in range(devices - 1)])
    f0, f1, f2, f3 = footage[0], footage[1], footage[2], footage[3]
    g = f3 - 0.5 * f2
    f4 = left(f0)
    g_prev = right(g)
    o1 = f1 - 0.5 * (f0 + f2)
    o3 = g - 0.5 * jnp.where(last, f2, f4)
    o_prev = jnp.where(first, o1, g_prev - 0.5 * f0)
    s0 = f0 + 0.25 * (o_prev + o1)
    s2 = f2 + 0.25 * (o1 + o3)
    h = s2 - 0.5 * s0
    s4 = left(s0)
    h_prev = right(h)
    d2 = h - 0.5 * jnp.where(last, s0, s4)
    d_prev = jnp.where(first, d2, h_prev - 0.5 * s0)
    t0 = s0 + 0.25 * (d_prev + d2)
    t_next = left(t0)
    t_prev = right(t0)
    p = t0 - 0.5 * t_prev
    high = p - 0.5 * jnp.where(last, t_prev, t_next)
    sent = jnp.where(odd, high, 0.0)
    hi_next = left(sent)
    hi_prev = right(sent)
    low = t0 + 0.25 * (jnp.where(first, hi_next, hi_prev) + hi_next)
    top = jnp.where(odd, high, low)
    coeffs = jnp.stack([top, o1, d2, o3])
    upper = lax.axis_index("row")
    strip = coeffs.shape[1]
    edge = jnp.where(upper == 0, coeffs[:, strip - HALO:], coeffs[:, :HALO])
    halos = lax.ppermute(edge, "row", [(0, 1), (1, 0)])
    out, energy = spatial_call(coeffs, halos)
    total = lax.psum(energy, ("frame", "row"))[:4, :3 * SLEVELS + 1]
    size = counts(4 * devices, strip * lax.axis_size("row"), footage.shape[2])
    return out, total / jnp.asarray(size, jnp.float32)


def solution(mesh):
    return jax.shard_map(
        shards,
        mesh=mesh,
        in_specs=(P("frame", "row", None),),
        out_specs=(P("frame", "row", None), P()),
        check_vma=False,
    )
```

```python
import functools

import jax
import jax.numpy as jnp
import ml_dtypes
import numpy as np
from jax import lax
from jax.experimental import pallas as pl
from jax.experimental.pallas import tpu as pltpu
from jax.sharding import PartitionSpec as P

SLEVELS = 3
TLEVELS = 3
ALPHA = -1.586134342
BETA = -0.05298011854
GAMMA = 0.8829110762
DELTA = 0.4435068522
ZETA = 1.149604398
HALO = 32
PAD = 8
LANES = 128
CHUNKS = 8


def lift_matrix(width):
    x = np.eye(width)
    e, o = x[:, 0::2], x[:, 1::2]
    after = lambda v: np.concatenate([v[:, 1:], v[:, -1:]], axis=1)
    before = lambda v: np.concatenate([v[:, :1], v[:, :-1]], axis=1)
    o = o + ALPHA * (e + after(e))
    e = e + BETA * (before(o) + o)
    o = o + GAMMA * (e + after(e))
    e = e + DELTA * (before(o) + o)
    out = np.zeros((width, width))
    out[:, 0::2] = e * ZETA
    out[:, 1::2] = o * (1.0 / ZETA)
    return out


def weight_blocks(width):
    levels = []
    for level in range(SLEVELS):
        s = 2**level
        m = np.zeros((width, width))
        m[::s, ::s] = lift_matrix(width // s)
        b = LANES
        mid = width // 2
        blocks = np.stack([
            m[:b, :b],
            m[mid:mid + b, mid:mid + b],
            m[width - b:, width - b:],
            m[mid - b:mid, mid:mid + b],
            m[mid + b:mid + 2 * b, mid:mid + b],
        ])
        hi = blocks.astype(ml_dtypes.bfloat16)
        lo = (blocks - hi.astype(np.float64)).astype(ml_dtypes.bfloat16)
        levels.append(np.stack([hi, lo]))
    return np.stack(levels)


TILES = (
    ((0, 3), (4, 1), (None, 4), (None, None)),
    ((3, None), (1, 3), (4, 1), (None, 4)),
    ((None, None), (3, None), (1, 3), (4, 2)),
)


def build_weights(blocks_ref, w_ref):
    zero = jnp.zeros((LANES, LANES), jnp.bfloat16)

    def fill(index, carry):
        level, part = index // 2, index % 2
        for kind in range(3):
            for r in range(4):
                for c in range(2):
                    which = TILES[kind][r][c]
                    value = zero if which is None else blocks_ref[level, part, which]
                    w_ref[level, part, kind, r * LANES:(r + 1) * LANES, c * LANES:(c + 1) * LANES] = value
        return carry

    lax.fori_loop(0, SLEVELS * 2, fill, 0)


def columns(xs, w_ref, level, store):
    count = len(xs)
    his, los = [], []
    for x in xs:
        hi = x.astype(jnp.bfloat16)
        his.append(hi)
        los.append((x - hi.astype(jnp.float32)).astype(jnp.bfloat16))
    for tile in range(count // 2):
        if tile == 0:
            kind, start = 0, 0
        elif tile == count // 2 - 1:
            kind, start = 2, count - 4
        else:
            kind, start = 1, 2 * tile - 1
        hi = jnp.concatenate(his[start:start + 4], axis=1)
        lo = jnp.concatenate(los[start:start + 4], axis=1)
        whi = w_ref[level, 0, kind]
        wlo = w_ref[level, 1, kind]
        dot = functools.partial(jnp.dot, preferred_element_type=jnp.float32)
        acc = dot(hi, whi) + dot(lo, whi) + dot(hi, wlo)
        store(2 * tile, acc[:, :LANES])
        store(2 * tile + 1, acc[:, LANES:])


def lift_rows(buf, pairs):
    ev = pl.ds(PAD, pairs, stride=2)
    od = pl.ds(PAD + 1, pairs, stride=2)
    ev_next = pl.ds(PAD + 2, pairs, stride=2)
    od_prev = pl.ds(PAD - 1, pairs, stride=2)
    end = PAD + 2 * pairs

    def panel(p, carry):
        def mirror_end():
            buf[p, end:end + 1, :] = buf[p, end - 2:end - 1, :]

        def mirror_start():
            buf[p, PAD - 1:PAD, :] = buf[p, PAD + 1:PAD + 2, :]

        mirror_end()
        buf[p, od, :] = buf[p, od, :] * (1.0 / ZETA) + (ALPHA / ZETA) * (buf[p, ev, :] + buf[p, ev_next, :])
        mirror_start()
        buf[p, ev, :] = buf[p, ev, :] + (BETA * ZETA) * (buf[p, od_prev, :] + buf[p, od, :])
        mirror_end()
        buf[p, od, :] = buf[p, od, :] + (GAMMA / ZETA) * (buf[p, ev, :] + buf[p, ev_next, :])
        mirror_start()
        buf[p, ev, :] = buf[p, ev, :] * ZETA + (DELTA * ZETA * ZETA) * (buf[p, od_prev, :] + buf[p, od, :])
        return carry

    lax.fori_loop(0, buf.shape[0], panel, 0)


def spatial(own, halo, upper, w_ref, bufs, before=None, midway=None):
    one, two, three = bufs
    panels = one.shape[0]
    rows = one.shape[1] - 2 * PAD
    strip = rows - HALO
    half = strip // 2
    own_at = pl.multiple_of(PAD + HALO * upper, 8)
    rest_at = pl.multiple_of(PAD + HALO * upper + half, 8)
    halo_at = pl.multiple_of(PAD + strip * (1 - upper), 8)

    def store_top(p, value):
        one[p, pl.ds(own_at, half), :] = value

    def store_rest(p, value):
        one[p, pl.ds(rest_at, half), :] = value[:half]
        one[p, pl.ds(halo_at, HALO), :] = value[half:]

    if before is not None:
        before()
    columns(own(0, half), w_ref, 0, store_top)
    rest = [jnp.concatenate(pair, axis=0) for pair in zip(own(half, half), halo())]
    columns(rest, w_ref, 0, store_rest)
    if midway is not None:
        midway()
    lift_rows(one, rows // 2)

    def into(buf, n):
        def store(p, value):
            buf[p, PAD:PAD + n, :] = value
        return store

    def evens(buf, n):
        return [buf[p, pl.ds(PAD, n, stride=2), :] for p in range(panels)]

    columns(evens(one, rows // 2), w_ref, 1, into(two, rows // 2))
    lift_rows(two, rows // 4)
    columns(evens(two, rows // 4), w_ref, 2, into(three, rows // 4))
    lift_rows(three, rows // 8)

    def merge(p, carry):
        lane = lax.broadcasted_iota(jnp.int32, (1, LANES), 1)
        n = rows // 4
        old = two[p, pl.ds(PAD, n, stride=2), :]
        two[p, pl.ds(PAD, n, stride=2), :] = jnp.where(lane % 4 == 0, three[p, PAD:PAD + n, :], old)
        n = rows // 2
        old = one[p, pl.ds(PAD, n, stride=2), :]
        one[p, pl.ds(PAD, n, stride=2), :] = jnp.where(lane % 2 == 0, two[p, PAD:PAD + n, :], old)
        return carry

    lax.fori_loop(0, panels, merge, 0)
    return own_at


def level_of(number, ceiling):
    depth = 1
    while number % 2 == 0 and depth <= ceiling:
        number //= 2
        depth += 1
    return depth


def band_of(row, col):
    u, v = level_of(row, SLEVELS), level_of(col, SLEVELS)
    m = min(u, v)
    if m > SLEVELS:
        return 3 * SLEVELS
    if u == v:
        return 3 * (m - 1) + 2
    return 3 * (m - 1) + (0 if u == m else 1)


def position_level(pos):
    return jnp.where(pos % 2 == 1, 1, jnp.where(pos % 4 == 2, 2, jnp.where(pos % 8 == 4, 3, 4)))


def band_table(shape):
    u = position_level(lax.broadcasted_iota(jnp.int32, shape, 0))
    v = position_level(lax.broadcasted_iota(jnp.int32, shape, 1))
    m = jnp.minimum(u, v)
    kind = jnp.where(u == v, 2, jnp.where(u == m, 0, 1))
    return jnp.where(m == SLEVELS + 1, 3 * SLEVELS, 3 * (m - 1) + kind)


def counts(frames, rows, cols):
    table = np.zeros(3 * SLEVELS + 1)
    for i in range(8):
        for j in range(8):
            table[band_of(i, j)] += 1 / 64
    share = np.array([0.5, 0.25, 0.125, 0.125])
    return float(frames) * rows * cols * np.outer(share, table)


def band_energy(one, at, strip, time_band):
    panels = one.shape[0]

    def panel(p, acc):
        value = one[p, pl.ds(at, strip), :]
        return acc + (value * value).reshape(-1, 8, LANES).sum(axis=0)

    total = lax.fori_loop(0, panels, panel, jnp.zeros((8, LANES), jnp.float32))
    bands = band_table((8, LANES))
    row = lax.broadcasted_iota(jnp.int32, (8, LANES), 0)
    col = lax.broadcasted_iota(jnp.int32, (8, LANES), 1)
    acc = jnp.zeros((8, LANES), jnp.float32)
    for s in range(3 * SLEVELS + 1):
        part = jnp.sum(jnp.where(bands == s, total, 0.0))
        acc = acc + jnp.where((row == time_band) & (col == s), part, 0.0)
    return acc


def panels_of(ref, width):
    def own(r, m):
        return [ref[r:r + m, p * LANES:(p + 1) * LANES] for p in range(width // LANES)]
    return own


def put_strip(one, at, strip, out_plane, sem):
    return [
        pltpu.make_async_copy(
            one.at[p, pl.ds(at, strip)], out_plane.at[:, p * LANES:(p + 1) * LANES], sem.at[p]
        )
        for p in range(one.shape[0])
    ]


def time_kernel(
    foot, blocks_ref, out, halo_out, energy_ref,
    f, recv, g, o1, o3, s0, h, d2, t0, top, edges, w_ref, one, two, three,
    in_sem, send_sem, recv_sem, edge_send, edge_recv, out_sem, top_sem, last_sem,
):
    strip, width = foot.shape[1:]
    me, upper = lax.axis_index("frame"), lax.axis_index("row")
    devices = lax.axis_size("frame")
    left, right = lax.rem(me + devices - 1, devices), lax.rem(me + 1, devices)
    first, last = me == 0, me == devices - 1
    odd = lax.rem(me, 2) == 1
    size = strip // CHUNKS

    def rows(c):
        at = jnp.where(upper == 1, c, CHUNKS - 1 - c) * size
        return pl.ds(pl.multiple_of(at, size), size)

    def send(level, side, c, src, where=None):
        return pltpu.make_async_remote_copy(
            src_ref=src.at[rows(c)],
            dst_ref=recv.at[level, side, rows(c)],
            send_sem=send_sem.at[level, side, c],
            recv_sem=recv_sem.at[level, side, c],
            device_id=(left if side == 0 else right, upper),
            device_id_type=pl.DeviceIdType.MESH,
        )

    def send_edge(plane, src):
        at = pl.multiple_of((strip - HALO) * (1 - upper), HALO)
        return pltpu.make_async_remote_copy(
            src_ref=src.at[pl.ds(at, HALO)],
            dst_ref=edges.at[plane],
            send_sem=edge_send.at[plane],
            recv_sem=edge_recv.at[plane],
            device_id=(me, 1 - upper),
            device_id_type=pl.DeviceIdType.MESH,
        )

    def each(body):
        def step(c, carry):
            body(c)
            return carry
        lax.fori_loop(0, CHUNKS, step, 0)

    loads = [pltpu.make_async_copy(foot.at[n], f.at[n], in_sem.at[n]) for n in range(4)]
    for n in (3, 2, 0, 1):
        loads[n].start()
    barrier = pltpu.get_barrier_semaphore()
    for where in ((left, upper), (right, upper), (me, 1 - upper)):
        pl.semaphore_signal(barrier, inc=1, device_id=where, device_id_type=pl.DeviceIdType.MESH)
    pl.semaphore_wait(barrier, 3)

    each(lambda c: send(0, 0, c, foot.at[0]).start())
    loads[3].wait()
    loads[2].wait()

    def first_right(c):
        r = rows(c)
        g[r] = f[3, r] - 0.5 * f[2, r]
        send(0, 1, c, g).start()

    each(first_right)
    loads[0].wait()
    loads[1].wait()

    def first_high(c):
        r = rows(c)
        o1[r] = f[1, r] - 0.5 * (f[0, r] + f[2, r])

    each(first_high)
    send_edge(0, o1).start()
    build_weights(blocks_ref, w_ref)
    bufs = (one, two, three)

    def plane_out(slot, src, frame, time_band, previous):
        def before():
            if previous is not None:
                for copy in previous:
                    copy.wait()

        def halo():
            send_edge(slot, src).wait_recv()
            return panels_of(edges.at[slot], width)(0, HALO)

        at = spatial(panels_of(src, width), halo, upper, w_ref, bufs, before)
        copies = put_strip(one, at, strip, out.at[frame], out_sem)
        for copy in copies:
            copy.start()
        return copies, band_energy(one, at, strip, time_band)

    copies, energy1 = plane_out(0, o1, 1, 0, None)

    def second(c):
        r = rows(c)
        send(0, 0, c, foot.at[0]).wait_recv()
        send(0, 1, c, g).wait_recv()
        f0, f2, first_o = f[0, r], f[2, r], o1[r]
        o_next = g[r] - 0.5 * jnp.where(last, f2, recv[0, 0, r])
        o_prev = jnp.where(first, first_o, recv[0, 1, r] - 0.5 * f0)
        low = f0 + 0.25 * (o_prev + first_o)
        o3[r] = o_next
        s0[r] = low
        h[r] = f2 + 0.25 * (first_o + o_next) - 0.5 * low
        send(1, 0, c, s0).start()
        send(1, 1, c, h).start()

        @pl.when(c == 0)
        def _():
            send_edge(1, o3).start()

    each(second)
    copies, energy3 = plane_out(1, o3, 3, 0, copies)

    def third(c):
        r = rows(c)
        send(1, 0, c, s0).wait_recv()
        send(1, 1, c, h).wait_recv()
        low = s0[r]
        high = h[r] - 0.5 * jnp.where(last, low, recv[1, 0, r])
        high_prev = jnp.where(first, high, recv[1, 1, r] - 0.5 * low)
        d2[r] = high
        t = low + 0.25 * (high_prev + high)

        @pl.when(jnp.logical_not(odd))
        def _():
            t0[r] = t
            send(2, 1, c, t0).start()
            send(2, 0, c, t0).start()

        @pl.when(odd)
        def _():
            send(2, 1, c, t0).wait_recv()
            t0[r] = t - 0.5 * recv[2, 1, r]
            send(2, 1, c, t0).start()

        @pl.when(c == 0)
        def _():
            send_edge(2, d2).start()

    each(third)
    copies, energy2 = plane_out(2, d2, 2, 1, copies)

    def fourth(c):
        r = rows(c)
        send(2, 0, c, t0).wait_recv()

        @pl.when(odd)
        def _():
            top[r] = t0[r] - 0.5 * jnp.where(last, recv[2, 1, r], recv[2, 0, r])
            send(2, 0, c, top).start()

        @pl.when(jnp.logical_not(odd))
        def _():
            send(2, 1, c, t0).wait_recv()
            mine, after = t0[r], recv[2, 0, r]
            prev = jnp.where(first, after, recv[2, 1, r] - 0.5 * mine)
            top[r] = mine + 0.25 * (prev + after)

        pltpu.make_async_copy(top.at[r], out.at[0, r], top_sem.at[c]).start()

        @pl.when(c == 0)
        def _():
            send_edge(3, top).start()

    each(fourth)
    energy_ref[...] = energy1 + energy2 + energy3
    send_edge(3, top).wait_recv()
    tail = pltpu.make_async_copy(edges.at[3], halo_out, last_sem)
    tail.start()
    for copy in copies:
        copy.wait()
    for plane, src in enumerate((o1, o3, d2, top)):
        send_edge(plane, src).wait_send()

    def drain(c):
        send(0, 0, c, foot.at[0]).wait_send()
        send(0, 1, c, g).wait_send()
        send(1, 0, c, s0).wait_send()
        send(1, 1, c, h).wait_send()
        send(2, 0, c, top).wait_send()
        send(2, 1, c, t0).wait_send()
        pltpu.make_async_copy(top.at[rows(c)], out.at[0, rows(c)], top_sem.at[c]).wait()

    each(drain)
    tail.wait()


def finish_kernel(planes, halo_ref, blocks_ref, part_ref, out, energy_ref, mine, stage, w_ref, one, two, three, in_sem, stage_sem, out_sem):
    strip, width = planes.shape[1:]
    upper = lax.axis_index("row")
    odd = lax.rem(lax.axis_index("frame"), 2) == 1
    load = pltpu.make_async_copy(planes.at[0], mine, in_sem)
    load.start()
    takes = [pltpu.make_async_copy(planes.at[n + 1], stage.at[n], stage_sem.at[0, n]) for n in range(3)]
    puts = [pltpu.make_async_copy(stage.at[n], out.at[n + 1], stage_sem.at[1, n]) for n in range(3)]
    for take in takes:
        take.start()
    build_weights(blocks_ref, w_ref)
    load.wait()

    def midway():
        for take, put in zip(takes, puts):
            take.wait()
            put.start()

    halo = lambda: panels_of(halo_ref, width)(0, HALO)
    at = spatial(panels_of(mine, width), halo, upper, w_ref, (one, two, three), midway=midway)
    copies = put_strip(one, at, strip, out.at[0], out_sem)
    for copy in copies:
        copy.start()
    energy_ref[...] = part_ref[...] + band_energy(one, at, strip, jnp.where(odd, 2, 3))
    for copy in copies + puts:
        copy.wait()


def spatial_scratch(strip, width):
    panels, rows = width // LANES, strip + HALO
    return [pltpu.VMEM((SLEVELS, 2, 3, 4 * LANES, 2 * LANES), jnp.bfloat16)] + [
        pltpu.VMEM((panels, rows // k + 2 * PAD, LANES), jnp.float32) for k in (1, 2, 4)
    ]


def shards(footage):
    frames, strip, width = footage.shape
    blocks = jnp.asarray(weight_blocks(width))
    plane = pltpu.VMEM((strip, width), jnp.float32)
    dma = pltpu.SemaphoreType.DMA
    full = jax.ShapeDtypeStruct(footage.shape, jnp.float32)
    tile = jax.ShapeDtypeStruct((8, LANES), jnp.float32)
    hbm = pl.BlockSpec(memory_space=pl.ANY)
    vmem = pl.BlockSpec(memory_space=pltpu.VMEM)
    planes, edge, part = pl.pallas_call(
        time_kernel,
        out_shape=(full, jax.ShapeDtypeStruct((HALO, width), jnp.float32), tile),
        in_specs=[hbm, vmem],
        out_specs=(hbm, hbm, vmem),
        scratch_shapes=[
            pltpu.VMEM(footage.shape, jnp.float32),
            pltpu.VMEM((3, 2, strip, width), jnp.float32),
            *[plane] * 8,
            pltpu.VMEM((4, HALO, width), jnp.float32),
            *spatial_scratch(strip, width),
            dma((4,)),
            dma((3, 2, CHUNKS)),
            dma((3, 2, CHUNKS)),
            dma((4,)),
            dma((4,)),
            dma((width // LANES,)),
            dma((CHUNKS,)),
            dma,
        ],
        compiler_params=pltpu.CompilerParams(
            collective_id=0, has_side_effects=True, vmem_limit_bytes=60 * 2**20
        ),
        name="time",
    )(footage, blocks)
    coeffs, energy = pl.pallas_call(
        finish_kernel,
        out_shape=(full, tile),
        in_specs=[hbm, vmem, vmem, vmem],
        out_specs=(hbm, vmem),
        scratch_shapes=[
            plane,
            pltpu.VMEM((3, strip, width), jnp.float32),
            *spatial_scratch(strip, width),
            dma,
            dma((2, 3)),
            dma((width // LANES,)),
        ],
        compiler_params=pltpu.CompilerParams(vmem_limit_bytes=40 * 2**20),
        name="finish",
    )(planes, edge, blocks, part)
    total = lax.psum(energy, ("frame", "row"))[:TLEVELS + 1, :3 * SLEVELS + 1]
    devices = lax.axis_size("frame")
    size = counts(frames * devices, strip * lax.axis_size("row"), width)
    return coeffs, total / jnp.asarray(size, jnp.float32)


def solution(mesh):
    return jax.shard_map(
        shards,
        mesh=mesh,
        in_specs=(P("frame", "row", None),),
        out_specs=(P("frame", "row", None), P()),
        check_vma=False,
    )
```

```python
import functools

import jax
import jax.numpy as jnp
import ml_dtypes
import numpy as np
from jax import lax
from jax.experimental import pallas as pl
from jax.experimental.pallas import tpu as pltpu
from jax.sharding import PartitionSpec as P

SLEVELS = 3
TLEVELS = 3
ALPHA = -1.586134342
BETA = -0.05298011854
GAMMA = 0.8829110762
DELTA = 0.4435068522
ZETA = 1.149604398
HALO = 32
PAD = 8
LANES = 128
CHUNKS = 8
Y_CHIPS = 4


def lift_matrix(width):
    x = np.eye(width)
    e, o = x[:, 0::2], x[:, 1::2]
    after = lambda v: np.concatenate([v[:, 1:], v[:, -1:]], axis=1)
    before = lambda v: np.concatenate([v[:, :1], v[:, :-1]], axis=1)
    o = o + ALPHA * (e + after(e))
    e = e + BETA * (before(o) + o)
    o = o + GAMMA * (e + after(e))
    e = e + DELTA * (before(o) + o)
    out = np.zeros((width, width))
    out[:, 0::2] = e * ZETA
    out[:, 1::2] = o * (1.0 / ZETA)
    return out


def weight_blocks(width):
    levels = []
    for level in range(SLEVELS):
        s = 2**level
        m = np.zeros((width, width))
        m[::s, ::s] = lift_matrix(width // s)
        b = LANES
        mid = width // 2
        blocks = np.stack([
            m[:b, :b],
            m[mid:mid + b, mid:mid + b],
            m[width - b:, width - b:],
            m[mid - b:mid, mid:mid + b],
            m[mid + b:mid + 2 * b, mid:mid + b],
        ])
        hi = blocks.astype(ml_dtypes.bfloat16)
        lo = (blocks - hi.astype(np.float64)).astype(ml_dtypes.bfloat16)
        levels.append(np.stack([hi, lo]))
    return np.stack(levels)


TILES = (
    ((0, 3), (4, 1), (None, 4), (None, None)),
    ((3, None), (1, 3), (4, 1), (None, 4)),
    ((None, None), (3, None), (1, 3), (4, 2)),
)


def build_weights(blocks_ref, w_ref):
    zero = jnp.zeros((LANES, LANES), jnp.bfloat16)

    def fill(index, carry):
        level, part = index // 2, index % 2
        for kind in range(3):
            for r in range(4):
                for c in range(2):
                    which = TILES[kind][r][c]
                    value = zero if which is None else blocks_ref[level, part, which]
                    w_ref[level, part, kind, r * LANES:(r + 1) * LANES, c * LANES:(c + 1) * LANES] = value
        return carry

    lax.fori_loop(0, SLEVELS * 2, fill, 0)


def columns(xs, w_ref, level, store):
    count = len(xs)
    his, los = [], []
    for x in xs:
        hi = x.astype(jnp.bfloat16)
        his.append(hi)
        los.append((x - hi.astype(jnp.float32)).astype(jnp.bfloat16))
    for tile in range(count // 2):
        if tile == 0:
            kind, start = 0, 0
        elif tile == count // 2 - 1:
            kind, start = 2, count - 4
        else:
            kind, start = 1, 2 * tile - 1
        hi = jnp.concatenate(his[start:start + 4], axis=1)
        lo = jnp.concatenate(los[start:start + 4], axis=1)
        whi = w_ref[level, 0, kind]
        wlo = w_ref[level, 1, kind]
        dot = functools.partial(jnp.dot, preferred_element_type=jnp.float32)
        acc = dot(hi, whi) + dot(lo, whi) + dot(hi, wlo)
        store(2 * tile, acc[:, :LANES])
        store(2 * tile + 1, acc[:, LANES:])


def lift_rows(buf, pairs):
    ev = pl.ds(PAD, pairs, stride=2)
    od = pl.ds(PAD + 1, pairs, stride=2)
    ev_next = pl.ds(PAD + 2, pairs, stride=2)
    od_prev = pl.ds(PAD - 1, pairs, stride=2)
    end = PAD + 2 * pairs

    def panel(p, carry):
        def mirror_end():
            buf[p, end:end + 1, :] = buf[p, end - 2:end - 1, :]

        def mirror_start():
            buf[p, PAD - 1:PAD, :] = buf[p, PAD + 1:PAD + 2, :]

        mirror_end()
        buf[p, od, :] = buf[p, od, :] * (1.0 / ZETA) + (ALPHA / ZETA) * (buf[p, ev, :] + buf[p, ev_next, :])
        mirror_start()
        buf[p, ev, :] = buf[p, ev, :] + (BETA * ZETA) * (buf[p, od_prev, :] + buf[p, od, :])
        mirror_end()
        buf[p, od, :] = buf[p, od, :] + (GAMMA / ZETA) * (buf[p, ev, :] + buf[p, ev_next, :])
        mirror_start()
        buf[p, ev, :] = buf[p, ev, :] * ZETA + (DELTA * ZETA * ZETA) * (buf[p, od_prev, :] + buf[p, od, :])
        return carry

    lax.fori_loop(0, buf.shape[0], panel, 0)


def strip_rows(one, upper):
    strip = one.shape[1] - 2 * PAD - HALO
    own_at = pl.multiple_of(PAD + HALO * upper, 8)
    halo_at = pl.multiple_of(PAD + strip * (1 - upper), 8)
    return strip, own_at, halo_at


def first_columns(own, halo, upper, w_ref, one):
    strip, own_at, halo_at = strip_rows(one, upper)
    half = strip // 2

    def store_top(p, value):
        one[p, pl.ds(own_at, half), :] = value

    def store_rest(p, value):
        one[p, pl.ds(pl.multiple_of(own_at + half, 8), half), :] = value[:half]
        one[p, pl.ds(halo_at, HALO), :] = value[half:]

    columns(own(0, half), w_ref, 0, store_top)
    rest = [jnp.concatenate(pair, axis=0) for pair in zip(own(half, half), halo())]
    columns(rest, w_ref, 0, store_rest)


def after_first_columns(w_ref, bufs):
    one, two, three = bufs
    panels = one.shape[0]
    rows = one.shape[1] - 2 * PAD
    lift_rows(one, rows // 2)

    def into(buf, n):
        def store(p, value):
            buf[p, PAD:PAD + n, :] = value
        return store

    def evens(buf, n):
        return [buf[p, pl.ds(PAD, n, stride=2), :] for p in range(panels)]

    columns(evens(one, rows // 2), w_ref, 1, into(two, rows // 2))
    lift_rows(two, rows // 4)
    columns(evens(two, rows // 4), w_ref, 2, into(three, rows // 4))
    lift_rows(three, rows // 8)

    def merge(p, carry):
        lane = lax.broadcasted_iota(jnp.int32, (1, LANES), 1)
        n = rows // 4
        old = two[p, pl.ds(PAD, n, stride=2), :]
        two[p, pl.ds(PAD, n, stride=2), :] = jnp.where(lane % 4 == 0, three[p, PAD:PAD + n, :], old)
        n = rows // 2
        old = one[p, pl.ds(PAD, n, stride=2), :]
        one[p, pl.ds(PAD, n, stride=2), :] = jnp.where(lane % 2 == 0, two[p, PAD:PAD + n, :], old)
        return carry

    lax.fori_loop(0, panels, merge, 0)


def level_of(number, ceiling):
    depth = 1
    while number % 2 == 0 and depth <= ceiling:
        number //= 2
        depth += 1
    return depth


def band_of(row, col):
    u, v = level_of(row, SLEVELS), level_of(col, SLEVELS)
    m = min(u, v)
    if m > SLEVELS:
        return 3 * SLEVELS
    if u == v:
        return 3 * (m - 1) + 2
    return 3 * (m - 1) + (0 if u == m else 1)


def position_level(pos):
    return jnp.where(pos % 2 == 1, 1, jnp.where(pos % 4 == 2, 2, jnp.where(pos % 8 == 4, 3, 4)))


def band_table(shape):
    u = position_level(lax.broadcasted_iota(jnp.int32, shape, 0))
    v = position_level(lax.broadcasted_iota(jnp.int32, shape, 1))
    m = jnp.minimum(u, v)
    kind = jnp.where(u == v, 2, jnp.where(u == m, 0, 1))
    return jnp.where(m == SLEVELS + 1, 3 * SLEVELS, 3 * (m - 1) + kind)


def counts(frames, rows, cols):
    table = np.zeros(3 * SLEVELS + 1)
    for i in range(8):
        for j in range(8):
            table[band_of(i, j)] += 1 / 64
    share = np.array([0.5, 0.25, 0.125, 0.125])
    return float(frames) * rows * cols * np.outer(share, table)


def band_energy(one, at, strip, time_band):
    panels = one.shape[0]

    def panel(p, acc):
        value = one[p, pl.ds(at, strip), :]
        return acc + (value * value).reshape(-1, 8, LANES).sum(axis=0)

    total = lax.fori_loop(0, panels, panel, jnp.zeros((8, LANES), jnp.float32))
    bands = band_table((8, LANES))
    row = lax.broadcasted_iota(jnp.int32, (8, LANES), 0)
    col = lax.broadcasted_iota(jnp.int32, (8, LANES), 1)
    acc = jnp.zeros((8, LANES), jnp.float32)
    for s in range(3 * SLEVELS + 1):
        part = jnp.sum(jnp.where(bands == s, total, 0.0))
        acc = acc + jnp.where((row == time_band) & (col == s), part, 0.0)
    return acc


def panels_of(ref, width):
    def own(r, m):
        return [ref[r:r + m, p * LANES:(p + 1) * LANES] for p in range(width // LANES)]
    return own


def put_strip(one, at, strip, out_plane, sem):
    return [
        pltpu.make_async_copy(
            one.at[p, pl.ds(at, strip)], out_plane.at[:, p * LANES:(p + 1) * LANES], sem.at[p]
        )
        for p in range(one.shape[0])
    ]


def time_kernel(
    foot, blocks_ref, counts_ref, out, energy_ref,
    f, recv, g, o1, o3, s0, h, d2, t0, top, edges, shared, w_ref, one, two, three,
    in_sem, send_sem, recv_sem, edge_send, edge_recv, out_sem, sum_send, sum_recv,
):
    strip, width = foot.shape[1:]
    me, upper = lax.axis_index("frame"), lax.axis_index("row")
    devices = lax.axis_size("frame")
    left, right = lax.rem(me + devices - 1, devices), lax.rem(me + 1, devices)
    first, last = me == 0, me == devices - 1
    odd = lax.rem(me, 2) == 1
    size = strip // CHUNKS

    def rows(c):
        at = jnp.where(upper == 1, c, CHUNKS - 1 - c) * size
        return pl.ds(pl.multiple_of(at, size), size)

    def send(level, side, c, src, where=None):
        return pltpu.make_async_remote_copy(
            src_ref=src.at[rows(c)],
            dst_ref=recv.at[level, side, rows(c)],
            send_sem=send_sem.at[level, side, c],
            recv_sem=recv_sem.at[level, side, c],
            device_id=(left if side == 0 else right, upper),
            device_id_type=pl.DeviceIdType.MESH,
        )

    def send_edge(plane, src):
        at = pl.multiple_of((strip - HALO) * (1 - upper), HALO)
        return pltpu.make_async_remote_copy(
            src_ref=src.at[pl.ds(at, HALO)],
            dst_ref=edges.at[plane],
            send_sem=edge_send.at[plane],
            recv_sem=edge_recv.at[plane],
            device_id=(me, 1 - upper),
            device_id_type=pl.DeviceIdType.MESH,
        )

    def each(body, begin=0, end=CHUNKS):
        def step(c, carry):
            body(c)
            return carry
        lax.fori_loop(begin, end, step, 0)

    ring = 2 * Y_CHIPS
    x_at, z_at, y_at = me // (2 * ring), lax.rem(me // ring, 2), lax.rem(me, ring)
    base = me - y_at
    groups = (
        (y_at, [(base + k, upper) for k in range(ring)]),
        (x_at, [(me + (k - x_at) * 2 * ring, upper) for k in range(devices // (2 * ring))]),
        (z_at + 2 * upper, [(me + (k % 2 - z_at) * ring, k // 2) for k in range(4)]),
    )

    loads = [pltpu.make_async_copy(foot.at[n], f.at[n], in_sem.at[n]) for n in range(4)]
    for n in (3, 2, 0, 1):
        loads[n].start()
    barrier = pltpu.get_barrier_semaphore()

    def greet(where):
        pl.semaphore_signal(barrier, inc=1, device_id=where, device_id_type=pl.DeviceIdType.MESH)

    for where in ((left, upper), (right, upper)):
        greet(where)
    for slot, members in groups:
        for k, where in enumerate(members):
            pl.when(slot != k)(functools.partial(greet, where))
    pl.semaphore_wait(barrier, 2 + sum(len(members) - 1 for _, members in groups))

    each(lambda c: send(0, 0, c, foot.at[0]).start())
    loads[3].wait()
    loads[2].wait()

    def first_right(c):
        r = rows(c)
        g[r] = f[3, r] - 0.5 * f[2, r]
        send(0, 1, c, g).start()

    each(first_right)
    loads[0].wait()
    loads[1].wait()

    def first_high(c):
        r = rows(c)
        o1[r] = f[1, r] - 0.5 * (f[0, r] + f[2, r])

    first_high(0)
    send_edge(0, o1).start()
    each(first_high, 1)
    build_weights(blocks_ref, w_ref)
    bufs = (one, two, three)

    def plane_out(slot, src, frame, time_band, previous):
        for copy in previous:
            copy.wait()

        def halo():
            send_edge(slot, src).wait_recv()
            return panels_of(edges.at[slot], width)(0, HALO)

        first_columns(panels_of(src, width), halo, upper, w_ref, one)
        return rest_out(frame, time_band)

    def rest_out(frame, time_band):
        after_first_columns(w_ref, bufs)
        own_at = strip_rows(one, upper)[1]
        copies = put_strip(one, own_at, strip, out.at[frame], out_sem)
        for copy in copies:
            copy.start()
        return copies, band_energy(one, own_at, strip, time_band)

    def second(c):
        r = rows(c)
        send(0, 0, c, foot.at[0]).wait_recv()
        send(0, 1, c, g).wait_recv()
        f0, f2, first_o = f[0, r], f[2, r], o1[r]
        o_next = g[r] - 0.5 * jnp.where(last, f2, recv[0, 0, r])
        o_prev = jnp.where(first, first_o, recv[0, 1, r] - 0.5 * f0)
        low = f0 + 0.25 * (o_prev + first_o)
        o3[r] = o_next
        s0[r] = low
        h[r] = f2 + 0.25 * (first_o + o_next) - 0.5 * low
        send(1, 0, c, s0).start()
        send(1, 1, c, h).start()

        @pl.when(c == 0)
        def _():
            send_edge(1, o3).start()

    each(second, 0, CHUNKS // 2)
    copies, energy1 = plane_out(0, o1, 1, 0, [])
    each(second, CHUNKS // 2)
    copies, energy3 = plane_out(1, o3, 3, 0, copies)

    def third(c):
        r = rows(c)
        send(1, 0, c, s0).wait_recv()
        send(1, 1, c, h).wait_recv()
        low = s0[r]
        high = h[r] - 0.5 * jnp.where(last, low, recv[1, 0, r])
        high_prev = jnp.where(first, high, recv[1, 1, r] - 0.5 * low)
        d2[r] = high
        t = low + 0.25 * (high_prev + high)

        @pl.when(jnp.logical_not(odd))
        def _():
            t0[r] = t
            send(2, 1, c, t0).start()
            send(2, 0, c, t0).start()

        @pl.when(odd)
        def _():
            send(2, 1, c, t0).wait_recv()
            t0[r] = t - 0.5 * recv[2, 1, r]
            send(2, 1, c, t0).start()

        @pl.when(c == 0)
        def _():
            send_edge(2, d2).start()

    each(third)
    copies, energy2 = plane_out(2, d2, 2, 1, copies)
    for copy in copies:
        copy.wait()
    own_at, halo_at = strip_rows(one, upper)[1:]

    def fourth(c):
        r = rows(c)
        send(2, 0, c, t0).wait_recv()

        @pl.when(odd)
        def _():
            top[r] = t0[r] - 0.5 * jnp.where(last, recv[2, 1, r], recv[2, 0, r])
            send(2, 0, c, top).start()

        @pl.when(jnp.logical_not(odd))
        def _():
            send(2, 1, c, t0).wait_recv()
            mine, after = t0[r], recv[2, 0, r]
            prev = jnp.where(first, after, recv[2, 1, r] - 0.5 * mine)
            top[r] = mine + 0.25 * (prev + after)

        @pl.when(c == 0)
        def _():
            send_edge(3, top).start()

        def store(p, value):
            one[p, pl.ds(pl.multiple_of(own_at + r.start, 8), size), :] = value

        columns([top[r, p * LANES:(p + 1) * LANES] for p in range(width // LANES)], w_ref, 0, store)

        @pl.when(c == CHUNKS - 2)
        def _():
            send_edge(3, top).wait_recv()

            def store_halo(p, value):
                one[p, pl.ds(halo_at, HALO), :] = value

            columns(panels_of(edges.at[3], width)(0, HALO), w_ref, 0, store_halo)

    each(fourth)
    copies, energy0 = rest_out(0, jnp.where(odd, 2, 3))
    total = energy0 + energy1 + energy2 + energy3

    def tell(stage, k):
        slot, members = groups[stage]
        return pltpu.make_async_remote_copy(
            src_ref=shared.at[stage, slot],
            dst_ref=shared.at[stage, slot],
            send_sem=sum_send.at[stage, k],
            recv_sem=sum_recv.at[stage, slot],
            device_id=members[k],
            device_id_type=pl.DeviceIdType.MESH,
        )

    def heard(stage, k):
        return pltpu.make_async_remote_copy(
            src_ref=shared.at[stage, k],
            dst_ref=shared.at[stage, k],
            send_sem=sum_send.at[stage, k],
            recv_sem=sum_recv.at[stage, k],
            device_id=groups[stage][1][k],
            device_id_type=pl.DeviceIdType.MESH,
        )

    for stage, (slot, members) in enumerate(groups):
        shared[stage, slot] = total
        for k in range(len(members)):
            pl.when(slot != k)(lambda stage=stage, k=k: tell(stage, k).start())
        for k in range(len(members)):
            pl.when(slot != k)(lambda stage=stage, k=k: heard(stage, k).wait_recv())
        total = functools.reduce(jnp.add, [shared[stage, k] for k in range(len(members))])
    energy_ref[...] = total[:TLEVELS + 1, :3 * SLEVELS + 1] / counts_ref[...]

    for stage, (slot, members) in enumerate(groups):
        for k in range(len(members)):
            pl.when(slot != k)(lambda stage=stage, k=k: tell(stage, k).wait_send())
    for copy in copies:
        copy.wait()
    for plane, src in enumerate((o1, o3, d2, top)):
        send_edge(plane, src).wait_send()

    def drain(c):
        send(0, 0, c, foot.at[0]).wait_send()
        send(0, 1, c, g).wait_send()
        send(1, 0, c, s0).wait_send()
        send(1, 1, c, h).wait_send()
        send(2, 0, c, top).wait_send()
        send(2, 1, c, t0).wait_send()

    each(drain)


def spatial_scratch(strip, width):
    panels, rows = width // LANES, strip + HALO
    return [pltpu.VMEM((SLEVELS, 2, 3, 4 * LANES, 2 * LANES), jnp.bfloat16)] + [
        pltpu.VMEM((panels, rows // k + 2 * PAD, LANES), jnp.float32) for k in (1, 2, 4)
    ]


def shards(footage):
    frames, strip, width = footage.shape
    blocks = jnp.asarray(weight_blocks(width))
    plane = pltpu.VMEM((strip, width), jnp.float32)
    dma = pltpu.SemaphoreType.DMA
    full = jax.ShapeDtypeStruct(footage.shape, jnp.float32)
    hbm = pl.BlockSpec(memory_space=pl.ANY)
    vmem = pl.BlockSpec(memory_space=pltpu.VMEM)
    devices = lax.axis_size("frame")
    size = counts(frames * devices, strip * lax.axis_size("row"), width)
    return pl.pallas_call(
        time_kernel,
        out_shape=(full, jax.ShapeDtypeStruct(size.shape, jnp.float32)),
        in_specs=[hbm, vmem, vmem],
        out_specs=(hbm, vmem),
        scratch_shapes=[
            pltpu.VMEM(footage.shape, jnp.float32),
            pltpu.VMEM((3, 2, strip, width), jnp.float32),
            *[plane] * 8,
            pltpu.VMEM((4, HALO, width), jnp.float32),
            pltpu.VMEM((3, 2 * Y_CHIPS, 8, LANES), jnp.float32),
            *spatial_scratch(strip, width),
            dma((4,)),
            dma((3, 2, CHUNKS)),
            dma((3, 2, CHUNKS)),
            dma((4,)),
            dma((4,)),
            dma((width // LANES,)),
            dma((3, 2 * Y_CHIPS)),
            dma((3, 2 * Y_CHIPS)),
        ],
        compiler_params=pltpu.CompilerParams(
            collective_id=0, has_side_effects=True, vmem_limit_bytes=60 * 2**20
        ),
        name="time",
    )(footage, blocks, jnp.asarray(size, jnp.float32))


def solution(mesh):
    return jax.shard_map(
        shards,
        mesh=mesh,
        in_specs=(P("frame", "row", None),),
        out_specs=(P("frame", "row", None), P()),
        check_vma=False,
    )
```

```python
import functools

import jax
import jax.numpy as jnp
import ml_dtypes
import numpy as np
from jax import lax
from jax.experimental import pallas as pl
from jax.experimental.pallas import tpu as pltpu
from jax.sharding import PartitionSpec as P

SLEVELS = 3
TLEVELS = 3
ALPHA = -1.586134342
BETA = -0.05298011854
GAMMA = 0.8829110762
DELTA = 0.4435068522
ZETA = 1.149604398
HALO = 32
PAD = 8
LANES = 128
CHUNKS = 8
RANK = 2 * SLEVELS
EXTRA = 8
Y_CHIPS = 4


def lift_matrix(width):
    x = np.eye(width)
    e, o = x[:, 0::2], x[:, 1::2]
    after = lambda v: np.concatenate([v[:, 1:], v[:, -1:]], axis=1)
    before = lambda v: np.concatenate([v[:, :1], v[:, :-1]], axis=1)
    o = o + ALPHA * (e + after(e))
    e = e + BETA * (before(o) + o)
    o = o + GAMMA * (e + after(e))
    e = e + DELTA * (before(o) + o)
    out = np.zeros((width, width))
    out[:, 0::2] = e * ZETA
    out[:, 1::2] = o * (1.0 / ZETA)
    return out


def weight_blocks(width):
    levels = []
    for level in range(SLEVELS):
        s = 2**level
        m = np.zeros((width, width))
        m[::s, ::s] = lift_matrix(width // s)
        b = LANES
        mid = width // 2
        blocks = np.stack([
            m[:b, :b],
            m[mid:mid + b, mid:mid + b],
            m[width - b:, width - b:],
            m[mid - b:mid, mid:mid + b],
            m[mid + b:mid + 2 * b, mid:mid + b],
        ])
        hi = blocks.astype(ml_dtypes.bfloat16)
        lo = (blocks - hi.astype(np.float64)).astype(ml_dtypes.bfloat16)
        levels.append(np.stack([hi, lo]))
    return np.stack(levels)


TILES = (
    ((0, 3), (4, 1), (None, 4), (None, None)),
    ((3, None), (1, 3), (4, 1), (None, 4)),
    ((None, None), (3, None), (1, 3), (4, 2)),
)


def summaries():
    n = 4 * HALO
    steps, done = [], np.eye(n)
    for level in range(SLEVELS):
        s = 2**level
        step = np.eye(n)
        step[::s, ::s] = lift_matrix(n // s).T
        done = step @ done
        steps.append(done)
    half = n // 2
    result = np.zeros((2, HALO, LANES))
    for side, (mine, other) in enumerate(((slice(half, n), slice(half - HALO, half)), (slice(0, half), slice(half, half + HALO)))):
        cross = np.concatenate([m[mine, other] for m in steps])
        basis = np.linalg.svd(cross)[2][:RANK]
        result[side, :, :RANK] = basis.T
    return result.astype(np.float32)


def build_weights(blocks_ref, w_ref):
    zero = jnp.zeros((LANES, LANES), jnp.bfloat16)

    def fill(index, carry):
        level, part = index // 2, index % 2
        for kind in range(3):
            for r in range(4):
                for c in range(2):
                    which = TILES[kind][r][c]
                    value = zero if which is None else blocks_ref[level, part, which]
                    w_ref[level, part, kind, r * LANES:(r + 1) * LANES, c * LANES:(c + 1) * LANES] = value
        return carry

    lax.fori_loop(0, SLEVELS * 2, fill, 0)


def columns(xs, w_ref, level, store):
    count = len(xs)
    his, los = [], []
    for x in xs:
        hi = x.astype(jnp.bfloat16)
        his.append(hi)
        los.append((x - hi.astype(jnp.float32)).astype(jnp.bfloat16))
    for tile in range(count // 2):
        if tile == 0:
            kind, start = 0, 0
        elif tile == count // 2 - 1:
            kind, start = 2, count - 4
        else:
            kind, start = 1, 2 * tile - 1
        hi = jnp.concatenate(his[start:start + 4], axis=1)
        lo = jnp.concatenate(los[start:start + 4], axis=1)
        whi = w_ref[level, 0, kind]
        wlo = w_ref[level, 1, kind]
        dot = functools.partial(jnp.dot, preferred_element_type=jnp.float32)
        acc = dot(hi, whi) + dot(lo, whi) + dot(hi, wlo)
        store(2 * tile, acc[:, :LANES])
        store(2 * tile + 1, acc[:, LANES:])


def lift_rows(buf, pairs):
    ev = pl.ds(PAD, pairs, stride=2)
    od = pl.ds(PAD + 1, pairs, stride=2)
    ev_next = pl.ds(PAD + 2, pairs, stride=2)
    od_prev = pl.ds(PAD - 1, pairs, stride=2)
    end = PAD + 2 * pairs

    def panel(p, carry):
        def mirror_end():
            buf[p, end:end + 1, :] = buf[p, end - 2:end - 1, :]

        def mirror_start():
            buf[p, PAD - 1:PAD, :] = buf[p, PAD + 1:PAD + 2, :]

        mirror_end()
        buf[p, od, :] = buf[p, od, :] * (1.0 / ZETA) + (ALPHA / ZETA) * (buf[p, ev, :] + buf[p, ev_next, :])
        mirror_start()
        buf[p, ev, :] = buf[p, ev, :] + (BETA * ZETA) * (buf[p, od_prev, :] + buf[p, od, :])
        mirror_end()
        buf[p, od, :] = buf[p, od, :] + (GAMMA / ZETA) * (buf[p, ev, :] + buf[p, ev_next, :])
        mirror_start()
        buf[p, ev, :] = buf[p, ev, :] * ZETA + (DELTA * ZETA * ZETA) * (buf[p, od_prev, :] + buf[p, od, :])
        return carry

    lax.fori_loop(0, buf.shape[0], panel, 0)


def strip_rows(one, upper):
    strip = one.shape[1] - 2 * PAD - HALO
    own_at = pl.multiple_of(PAD + HALO * upper, 8)
    halo_at = pl.multiple_of(PAD + strip * (1 - upper), 8)
    return strip, own_at, halo_at


def first_columns(own, halo, upper, w_ref, one):
    strip, own_at, halo_at = strip_rows(one, upper)
    half = strip // 2

    def store_top(p, value):
        one[p, pl.ds(own_at, half), :] = value

    def store_rest(p, value):
        one[p, pl.ds(pl.multiple_of(own_at + half, 8), half), :] = value[:half]
        one[p, pl.ds(halo_at, HALO), :] = value[half:]

    columns(own(0, half), w_ref, 0, store_top)
    rest = [jnp.concatenate(pair, axis=0) for pair in zip(own(half, half), halo())]
    columns(rest, w_ref, 0, store_rest)


def after_first_columns(w_ref, bufs):
    one, two, three = bufs
    panels = one.shape[0]
    rows = one.shape[1] - 2 * PAD
    lift_rows(one, rows // 2)

    def into(buf, n):
        def store(p, value):
            buf[p, PAD:PAD + n, :] = value
        return store

    def evens(buf, n):
        return [buf[p, pl.ds(PAD, n, stride=2), :] for p in range(panels)]

    columns(evens(one, rows // 2), w_ref, 1, into(two, rows // 2))
    lift_rows(two, rows // 4)
    columns(evens(two, rows // 4), w_ref, 2, into(three, rows // 4))
    lift_rows(three, rows // 8)

    def merge(p, carry):
        lane = lax.broadcasted_iota(jnp.int32, (1, LANES), 1)
        n = rows // 4
        old = two[p, pl.ds(PAD, n, stride=2), :]
        two[p, pl.ds(PAD, n, stride=2), :] = jnp.where(lane % 4 == 0, three[p, PAD:PAD + n, :], old)
        n = rows // 2
        old = one[p, pl.ds(PAD, n, stride=2), :]
        one[p, pl.ds(PAD, n, stride=2), :] = jnp.where(lane % 2 == 0, two[p, PAD:PAD + n, :], old)
        return carry

    lax.fori_loop(0, panels, merge, 0)


def level_of(number, ceiling):
    depth = 1
    while number % 2 == 0 and depth <= ceiling:
        number //= 2
        depth += 1
    return depth


def band_of(row, col):
    u, v = level_of(row, SLEVELS), level_of(col, SLEVELS)
    m = min(u, v)
    if m > SLEVELS:
        return 3 * SLEVELS
    if u == v:
        return 3 * (m - 1) + 2
    return 3 * (m - 1) + (0 if u == m else 1)


def position_level(pos):
    return jnp.where(pos % 2 == 1, 1, jnp.where(pos % 4 == 2, 2, jnp.where(pos % 8 == 4, 3, 4)))


def band_table(shape):
    u = position_level(lax.broadcasted_iota(jnp.int32, shape, 0))
    v = position_level(lax.broadcasted_iota(jnp.int32, shape, 1))
    m = jnp.minimum(u, v)
    kind = jnp.where(u == v, 2, jnp.where(u == m, 0, 1))
    return jnp.where(m == SLEVELS + 1, 3 * SLEVELS, 3 * (m - 1) + kind)


def counts(frames, rows, cols):
    table = np.zeros(3 * SLEVELS + 1)
    for i in range(8):
        for j in range(8):
            table[band_of(i, j)] += 1 / 64
    share = np.array([0.5, 0.25, 0.125, 0.125])
    return float(frames) * rows * cols * np.outer(share, table)


def band_energy(one, at, strip, time_band):
    panels = one.shape[0]

    def panel(p, acc):
        value = one[p, pl.ds(at, strip), :]
        return acc + (value * value).reshape(-1, 8, LANES).sum(axis=0)

    total = lax.fori_loop(0, panels, panel, jnp.zeros((8, LANES), jnp.float32))
    bands = band_table((8, LANES))
    row = lax.broadcasted_iota(jnp.int32, (8, LANES), 0)
    col = lax.broadcasted_iota(jnp.int32, (8, LANES), 1)
    acc = jnp.zeros((8, LANES), jnp.float32)
    for s in range(3 * SLEVELS + 1):
        part = jnp.sum(jnp.where(bands == s, total, 0.0))
        acc = acc + jnp.where((row == time_band) & (col == s), part, 0.0)
    return acc


def panels_of(ref, width):
    def own(r, m):
        return [ref[r:r + m, p * LANES:(p + 1) * LANES] for p in range(width // LANES)]
    return own


def put_strip(one, at, strip, out_plane, sem):
    return [
        pltpu.make_async_copy(
            one.at[p, pl.ds(at, strip)], out_plane.at[:, p * LANES:(p + 1) * LANES], sem.at[p]
        )
        for p in range(one.shape[0])
    ]


def time_kernel(
    foot, blocks_ref, basis_ref, counts_ref, out, energy_ref,
    f, recv, g, o1, o3, s0, h, d2, t0, top, border, summary, shared, w_ref, one, two, three,
    in_sem, border_sem, send_sem, recv_sem, across, out_sem, sum_send, sum_recv,
):
    strip, width = foot.shape[1:]
    me, upper = lax.axis_index("frame"), lax.axis_index("row")
    devices = lax.axis_size("frame")
    left, right = lax.rem(me + devices - 1, devices), lax.rem(me + 1, devices)
    first, last = me == 0, me == devices - 1
    odd = lax.rem(me, 2) == 1
    size = strip // CHUNKS

    def rows(c):
        if isinstance(c, int) and c == CHUNKS:
            return pl.ds(strip, EXTRA)
        return pl.ds(pl.multiple_of(c * size, size), size)

    def send(level, side, c, src):
        return pltpu.make_async_remote_copy(
            src_ref=src.at[rows(c)],
            dst_ref=recv.at[level, side, rows(c)],
            send_sem=send_sem.at[level, side, c],
            recv_sem=recv_sem.at[level, side, c],
            device_id=(left if side == 0 else right, upper),
            device_id_type=pl.DeviceIdType.MESH,
        )

    def each(body, begin=0, end=CHUNKS):
        def step(c, carry):
            body(c)
            return carry
        lax.fori_loop(begin, end, step, 0)

    ring = 2 * Y_CHIPS
    x_at, z_at, y_at = me // (2 * ring), lax.rem(me // ring, 2), lax.rem(me, ring)
    base = me - y_at
    groups = (
        (y_at, [(base + k, upper) for k in range(ring)]),
        (x_at, [(me + (k - x_at) * 2 * ring, upper) for k in range(devices // (2 * ring))]),
        (z_at + 2 * upper, [(me + (k % 2 - z_at) * ring, k // 2) for k in range(4)]),
    )

    border_at = pl.multiple_of((strip - HALO) * (1 - upper), HALO)
    borders = pltpu.make_async_copy(foot.at[:, pl.ds(border_at, HALO)], border, border_sem)
    borders.start()
    loads = [pltpu.make_async_copy(foot.at[n], f.at[n, pl.ds(0, strip)], in_sem.at[n]) for n in range(4)]
    for n in (3, 2, 0, 1):
        loads[n].start()
    barrier = pltpu.get_barrier_semaphore()

    def greet(where):
        pl.semaphore_signal(barrier, inc=1, device_id=where, device_id_type=pl.DeviceIdType.MESH)

    for where in ((left, upper), (right, upper)):
        greet(where)
    for slot, members in groups:
        for k, where in enumerate(members):
            pl.when(slot != k)(functools.partial(greet, where))

    borders.wait()
    for n in range(4):
        values = border[n]
        for k in range(RANK):
            summary[n, k:k + 1, :] = (basis_ref[upper, :, k:k + 1] * values).sum(axis=0, keepdims=True)
        summary[n, RANK:, :] = jnp.zeros((EXTRA - RANK, width), jnp.float32)
    exchange = pltpu.make_async_remote_copy(
        src_ref=summary,
        dst_ref=f.at[:, pl.ds(strip, EXTRA)],
        send_sem=across.at[0],
        recv_sem=across.at[1],
        device_id=(me, 1 - upper),
        device_id_type=pl.DeviceIdType.MESH,
    )
    pl.semaphore_wait(barrier, 2 + sum(len(members) - 1 for _, members in groups))
    exchange.start()

    def first_left():
        each(lambda c: send(0, 0, c, foot.at[0]).start())

    def first_right():
        each(lambda c: send(0, 1, c, g).start())

    def partial(c):
        r = rows(c)
        g[r] = f[3, r] - 0.5 * f[2, r]

    def first_high(c):
        r = rows(c)
        o1[r] = f[1, r] - 0.5 * (f[0, r] + f[2, r])

    pl.when(y_at != 0)(first_left)
    loads[3].wait()
    loads[2].wait()
    each(partial)
    pl.when(y_at != ring - 1)(first_right)
    loads[0].wait()
    loads[1].wait()
    each(first_high)
    exchange.wait_recv()
    pl.when(y_at == 0)(first_left)
    pl.when(y_at == ring - 1)(first_right)
    partial(CHUNKS)
    first_high(CHUNKS)
    send(0, 0, CHUNKS, f.at[0]).start()
    send(0, 1, CHUNKS, g).start()
    build_weights(blocks_ref, w_ref)
    bufs = (one, two, three)

    def halo_of(src):
        values = src[rows(CHUNKS)]
        total = basis_ref[1 - upper, :, 0:1] * values[0:1]
        for k in range(1, RANK):
            total = total + basis_ref[1 - upper, :, k:k + 1] * values[k:k + 1]
        return [total[:, p * LANES:(p + 1) * LANES] for p in range(width // LANES)]

    def plane_out(src, frame, time_band, previous):
        for copy in previous:
            copy.wait()
        first_columns(panels_of(src, width), lambda: halo_of(src), upper, w_ref, one)
        return rest_out(frame, time_band)

    def rest_out(frame, time_band):
        after_first_columns(w_ref, bufs)
        own_at = strip_rows(one, upper)[1]
        copies = put_strip(one, own_at, strip, out.at[frame], out_sem)
        for copy in copies:
            copy.start()
        return copies, band_energy(one, own_at, strip, time_band)

    def second(c):
        r = rows(c)
        send(0, 0, c, g).wait_recv()
        send(0, 1, c, g).wait_recv()
        f0, f2, first_o = f[0, r], f[2, r], o1[r]
        o_next = g[r] - 0.5 * jnp.where(last, f2, recv[0, 0, r])
        o_prev = jnp.where(first, first_o, recv[0, 1, r] - 0.5 * f0)
        low = f0 + 0.25 * (o_prev + first_o)
        o3[r] = o_next
        s0[r] = low
        h[r] = f2 + 0.25 * (first_o + o_next) - 0.5 * low
        send(1, 0, c, s0).start()
        send(1, 1, c, h).start()

    def third(c):
        r = rows(c)
        send(1, 0, c, s0).wait_recv()
        send(1, 1, c, h).wait_recv()
        low = s0[r]
        high = h[r] - 0.5 * jnp.where(last, low, recv[1, 0, r])
        high_prev = jnp.where(first, high, recv[1, 1, r] - 0.5 * low)
        d2[r] = high
        t = low + 0.25 * (high_prev + high)

        @pl.when(jnp.logical_not(odd))
        def _():
            t0[r] = t
            send(2, 1, c, t0).start()
            send(2, 0, c, t0).start()

        @pl.when(odd)
        def _():
            send(2, 1, c, t0).wait_recv()
            t0[r] = t - 0.5 * recv[2, 1, r]
            send(2, 1, c, t0).start()

    def fourth(c):
        r = rows(c)
        send(2, 0, c, t0).wait_recv()

        @pl.when(odd)
        def _():
            top[r] = t0[r] - 0.5 * jnp.where(last, recv[2, 1, r], recv[2, 0, r])
            send(2, 0, c, top).start()

        @pl.when(jnp.logical_not(odd))
        def _():
            send(2, 1, c, t0).wait_recv()
            mine, after = t0[r], recv[2, 0, r]
            prev = jnp.where(first, after, recv[2, 1, r] - 0.5 * mine)
            top[r] = mine + 0.25 * (prev + after)

    copies, energy1 = plane_out(o1, 1, 0, [])
    each(second)
    second(CHUNKS)
    copies, energy3 = plane_out(o3, 3, 0, copies)
    each(third)
    third(CHUNKS)
    copies, energy2 = plane_out(d2, 2, 1, copies)
    for copy in copies:
        copy.wait()
    own_at, halo_at = strip_rows(one, upper)[1:]

    def panels_at(r):
        return [top[r, p * LANES:(p + 1) * LANES] for p in range(width // LANES)]

    def finish(c):
        fourth(c)

        def store(p, value):
            one[p, pl.ds(pl.multiple_of(own_at + c * size, 8), size), :] = value

        columns(panels_at(rows(c)), w_ref, 0, store)

    each(finish, 0, CHUNKS - 1)
    fourth(CHUNKS - 1)
    fourth(CHUNKS)

    def store(p, value):
        one[p, pl.ds(pl.multiple_of(own_at + strip - size, 8), size), :] = value[:size]
        one[p, pl.ds(halo_at, HALO), :] = value[size:]

    ends = [jnp.concatenate(pair, axis=0) for pair in zip(panels_at(rows(CHUNKS - 1)), halo_of(top))]
    columns(ends, w_ref, 0, store)
    copies, energy0 = rest_out(0, jnp.where(odd, 2, 3))
    total = energy0 + energy1 + energy2 + energy3

    def tell(stage, k):
        slot, members = groups[stage]
        return pltpu.make_async_remote_copy(
            src_ref=shared.at[stage, slot],
            dst_ref=shared.at[stage, slot],
            send_sem=sum_send.at[stage, k],
            recv_sem=sum_recv.at[stage, slot],
            device_id=members[k],
            device_id_type=pl.DeviceIdType.MESH,
        )

    def heard(stage, k):
        return pltpu.make_async_remote_copy(
            src_ref=shared.at[stage, k],
            dst_ref=shared.at[stage, k],
            send_sem=sum_send.at[stage, k],
            recv_sem=sum_recv.at[stage, k],
            device_id=groups[stage][1][k],
            device_id_type=pl.DeviceIdType.MESH,
        )

    for stage, (slot, members) in enumerate(groups):
        shared[stage, slot] = total
        for k in range(len(members)):
            pl.when(slot != k)(lambda stage=stage, k=k: tell(stage, k).start())
        for k in range(len(members)):
            pl.when(slot != k)(lambda stage=stage, k=k: heard(stage, k).wait_recv())
        total = functools.reduce(jnp.add, [shared[stage, k] for k in range(len(members))])
    energy_ref[...] = total[:TLEVELS + 1, :3 * SLEVELS + 1] / counts_ref[...]

    for stage, (slot, members) in enumerate(groups):
        for k in range(len(members)):
            pl.when(slot != k)(lambda stage=stage, k=k: tell(stage, k).wait_send())
    for copy in copies:
        copy.wait()
    exchange.wait_send()

    def drain(c):
        send(0, 0, c, g).wait_send()
        send(0, 1, c, g).wait_send()
        send(1, 0, c, s0).wait_send()
        send(1, 1, c, h).wait_send()
        send(2, 0, c, top).wait_send()
        send(2, 1, c, t0).wait_send()

    each(drain)
    drain(CHUNKS)


def spatial_scratch(strip, width):
    panels, rows = width // LANES, strip + HALO
    return [pltpu.VMEM((SLEVELS, 2, 3, 4 * LANES, 2 * LANES), jnp.bfloat16)] + [
        pltpu.VMEM((panels, rows // k + 2 * PAD, LANES), jnp.float32) for k in (1, 2, 4)
    ]


def shards(footage):
    frames, strip, width = footage.shape
    blocks = jnp.asarray(weight_blocks(width))
    plane = pltpu.VMEM((strip + EXTRA, width), jnp.float32)
    dma = pltpu.SemaphoreType.DMA
    full = jax.ShapeDtypeStruct(footage.shape, jnp.float32)
    hbm = pl.BlockSpec(memory_space=pl.ANY)
    vmem = pl.BlockSpec(memory_space=pltpu.VMEM)
    devices = lax.axis_size("frame")
    size = counts(frames * devices, strip * lax.axis_size("row"), width)
    return pl.pallas_call(
        time_kernel,
        out_shape=(full, jax.ShapeDtypeStruct(size.shape, jnp.float32)),
        in_specs=[hbm, vmem, vmem, vmem],
        out_specs=(hbm, vmem),
        scratch_shapes=[
            pltpu.VMEM((frames, strip + EXTRA, width), jnp.float32),
            pltpu.VMEM((3, 2, strip + EXTRA, width), jnp.float32),
            *[plane] * 8,
            pltpu.VMEM((frames, HALO, width), jnp.float32),
            pltpu.VMEM((frames, EXTRA, width), jnp.float32),
            pltpu.VMEM((3, 2 * Y_CHIPS, 8, LANES), jnp.float32),
            *spatial_scratch(strip, width),
            dma((4,)),
            dma,
            dma((3, 2, CHUNKS + 1)),
            dma((3, 2, CHUNKS + 1)),
            dma((2,)),
            dma((width // LANES,)),
            dma((3, 2 * Y_CHIPS)),
            dma((3, 2 * Y_CHIPS)),
        ],
        compiler_params=pltpu.CompilerParams(
            collective_id=0, has_side_effects=True, vmem_limit_bytes=60 * 2**20
        ),
        name="time",
    )(footage, blocks, jnp.asarray(summaries()), jnp.asarray(size, jnp.float32))


def solution(mesh):
    return jax.shard_map(
        shards,
        mesh=mesh,
        in_specs=(P("frame", "row", None),),
        out_specs=(P("frame", "row", None), P()),
        check_vma=False,
    )
```

```python
import functools

import jax
import jax.numpy as jnp
import ml_dtypes
import numpy as np
from jax import lax
from jax.experimental import pallas as pl
from jax.experimental.pallas import tpu as pltpu
from jax.sharding import PartitionSpec as P

SLEVELS = 3
TLEVELS = 3
ALPHA = -1.586134342
BETA = -0.05298011854
GAMMA = 0.8829110762
DELTA = 0.4435068522
ZETA = 1.149604398
HALO = 32
PAD = 8
LANES = 128
CHUNKS = 8
RANK = 2 * SLEVELS
EXTRA = 8
Y_CHIPS = 4


def lift_matrix(width):
    x = np.eye(width)
    e, o = x[:, 0::2], x[:, 1::2]
    after = lambda v: np.concatenate([v[:, 1:], v[:, -1:]], axis=1)
    before = lambda v: np.concatenate([v[:, :1], v[:, :-1]], axis=1)
    o = o + ALPHA * (e + after(e))
    e = e + BETA * (before(o) + o)
    o = o + GAMMA * (e + after(e))
    e = e + DELTA * (before(o) + o)
    out = np.zeros((width, width))
    out[:, 0::2] = e * ZETA
    out[:, 1::2] = o * (1.0 / ZETA)
    return out


def weight_blocks(width):
    levels = []
    for level in range(SLEVELS):
        s = 2**level
        m = np.zeros((width, width))
        m[::s, ::s] = lift_matrix(width // s)
        b = LANES
        mid = width // 2
        blocks = np.stack([
            m[:b, :b],
            m[mid:mid + b, mid:mid + b],
            m[width - b:, width - b:],
            m[mid - b:mid, mid:mid + b],
            m[mid + b:mid + 2 * b, mid:mid + b],
        ])
        hi = blocks.astype(ml_dtypes.bfloat16)
        lo = (blocks - hi.astype(np.float64)).astype(ml_dtypes.bfloat16)
        levels.append(np.stack([hi, lo]))
    return np.stack(levels)


TILES = (
    ((0, 3), (4, 1), (None, 4), (None, None)),
    ((3, None), (1, 3), (4, 1), (None, 4)),
    ((None, None), (3, None), (1, 3), (4, 2)),
)


def summaries():
    n = 4 * HALO
    steps, done = [], np.eye(n)
    for level in range(SLEVELS):
        s = 2**level
        step = np.eye(n)
        step[::s, ::s] = lift_matrix(n // s).T
        done = step @ done
        steps.append(done)
    half = n // 2
    result = np.zeros((2, HALO, LANES))
    for side, (mine, other) in enumerate(((slice(half, n), slice(half - HALO, half)), (slice(0, half), slice(half, half + HALO)))):
        cross = np.concatenate([m[mine, other] for m in steps])
        basis = np.linalg.svd(cross)[2][:RANK]
        result[side, :, :RANK] = basis.T
    return result.astype(np.float32)


def build_weights(blocks_ref, w_ref):
    zero = jnp.zeros((LANES, LANES), jnp.bfloat16)

    def fill(index, carry):
        level, part = index // 2, index % 2
        for kind in range(3):
            for r in range(4):
                for c in range(2):
                    which = TILES[kind][r][c]
                    value = zero if which is None else blocks_ref[level, part, which]
                    w_ref[level, part, kind, r * LANES:(r + 1) * LANES, c * LANES:(c + 1) * LANES] = value
        return carry

    lax.fori_loop(0, SLEVELS * 2, fill, 0)


def columns(xs, w_ref, level, store):
    count = len(xs)
    his, los = [], []
    for x in xs:
        hi = x.astype(jnp.bfloat16)
        his.append(hi)
        los.append((x - hi.astype(jnp.float32)).astype(jnp.bfloat16))
    for tile in range(count // 2):
        if tile == 0:
            kind, start = 0, 0
        elif tile == count // 2 - 1:
            kind, start = 2, count - 4
        else:
            kind, start = 1, 2 * tile - 1
        hi = jnp.concatenate(his[start:start + 4], axis=1)
        lo = jnp.concatenate(los[start:start + 4], axis=1)
        whi = w_ref[level, 0, kind]
        wlo = w_ref[level, 1, kind]
        dot = functools.partial(jnp.dot, preferred_element_type=jnp.float32)
        acc = dot(hi, whi) + dot(lo, whi) + dot(hi, wlo)
        store(2 * tile, acc[:, :LANES])
        store(2 * tile + 1, acc[:, LANES:])


def lift_rows(buf, pairs):
    ev = pl.ds(PAD, pairs, stride=2)
    od = pl.ds(PAD + 1, pairs, stride=2)
    ev_next = pl.ds(PAD + 2, pairs, stride=2)
    od_prev = pl.ds(PAD - 1, pairs, stride=2)
    end = PAD + 2 * pairs

    def panel(p, carry):
        def mirror_end():
            buf[p, end:end + 1, :] = buf[p, end - 2:end - 1, :]

        def mirror_start():
            buf[p, PAD - 1:PAD, :] = buf[p, PAD + 1:PAD + 2, :]

        mirror_end()
        buf[p, od, :] = buf[p, od, :] * (1.0 / ZETA) + (ALPHA / ZETA) * (buf[p, ev, :] + buf[p, ev_next, :])
        mirror_start()
        buf[p, ev, :] = buf[p, ev, :] + (BETA * ZETA) * (buf[p, od_prev, :] + buf[p, od, :])
        mirror_end()
        buf[p, od, :] = buf[p, od, :] + (GAMMA / ZETA) * (buf[p, ev, :] + buf[p, ev_next, :])
        mirror_start()
        buf[p, ev, :] = buf[p, ev, :] * ZETA + (DELTA * ZETA * ZETA) * (buf[p, od_prev, :] + buf[p, od, :])
        return carry

    lax.fori_loop(0, buf.shape[0], panel, 0, unroll=2)


def strip_rows(one, upper):
    strip = one.shape[1] - 2 * PAD - HALO
    own_at = pl.multiple_of(PAD + HALO * upper, 8)
    halo_at = pl.multiple_of(PAD + strip * (1 - upper), 8)
    return strip, own_at, halo_at


def first_columns(own, halo, upper, w_ref, one):
    strip, own_at, halo_at = strip_rows(one, upper)
    half = strip // 2

    def store_top(p, value):
        one[p, pl.ds(own_at, half), :] = value

    def store_rest(p, value):
        one[p, pl.ds(pl.multiple_of(own_at + half, 8), half), :] = value[:half]
        one[p, pl.ds(halo_at, HALO), :] = value[half:]

    columns(own(0, half), w_ref, 0, store_top)
    rest = [jnp.concatenate(pair, axis=0) for pair in zip(own(half, half), halo())]
    columns(rest, w_ref, 0, store_rest)


def after_first_columns(w_ref, bufs):
    one, two, three = bufs
    panels = one.shape[0]
    rows = one.shape[1] - 2 * PAD
    lift_rows(one, rows // 2)

    def into(buf, n):
        def store(p, value):
            buf[p, PAD:PAD + n, :] = value
        return store

    def evens(buf, n):
        return [buf[p, pl.ds(PAD, n, stride=2), :] for p in range(panels)]

    columns(evens(one, rows // 2), w_ref, 1, into(two, rows // 2))
    lift_rows(two, rows // 4)
    columns(evens(two, rows // 4), w_ref, 2, into(three, rows // 4))
    lift_rows(three, rows // 8)

    def merge(p, carry):
        lane = lax.broadcasted_iota(jnp.int32, (1, LANES), 1)
        n = rows // 4
        old = two[p, pl.ds(PAD, n, stride=2), :]
        two[p, pl.ds(PAD, n, stride=2), :] = jnp.where(lane % 4 == 0, three[p, PAD:PAD + n, :], old)
        n = rows // 2
        old = one[p, pl.ds(PAD, n, stride=2), :]
        one[p, pl.ds(PAD, n, stride=2), :] = jnp.where(lane % 2 == 0, two[p, PAD:PAD + n, :], old)
        return carry

    lax.fori_loop(0, panels, merge, 0, unroll=2)


def level_of(number, ceiling):
    depth = 1
    while number % 2 == 0 and depth <= ceiling:
        number //= 2
        depth += 1
    return depth


def band_of(row, col):
    u, v = level_of(row, SLEVELS), level_of(col, SLEVELS)
    m = min(u, v)
    if m > SLEVELS:
        return 3 * SLEVELS
    if u == v:
        return 3 * (m - 1) + 2
    return 3 * (m - 1) + (0 if u == m else 1)


def position_level(pos):
    return jnp.where(pos % 2 == 1, 1, jnp.where(pos % 4 == 2, 2, jnp.where(pos % 8 == 4, 3, 4)))


def band_table(shape):
    u = position_level(lax.broadcasted_iota(jnp.int32, shape, 0))
    v = position_level(lax.broadcasted_iota(jnp.int32, shape, 1))
    m = jnp.minimum(u, v)
    kind = jnp.where(u == v, 2, jnp.where(u == m, 0, 1))
    return jnp.where(m == SLEVELS + 1, 3 * SLEVELS, 3 * (m - 1) + kind)


def counts(frames, rows, cols):
    table = np.zeros(3 * SLEVELS + 1)
    for i in range(8):
        for j in range(8):
            table[band_of(i, j)] += 1 / 64
    share = np.array([0.5, 0.25, 0.125, 0.125])
    return float(frames) * rows * cols * np.outer(share, table)


def band_energy(one, at, strip, time_band):
    panels = one.shape[0]

    def panel(p, acc):
        value = one[p, pl.ds(at, strip), :]
        return acc + (value * value).reshape(-1, 8, LANES).sum(axis=0)

    total = lax.fori_loop(0, panels, panel, jnp.zeros((8, LANES), jnp.float32), unroll=2)
    bands = band_table((8, LANES))
    row = lax.broadcasted_iota(jnp.int32, (8, LANES), 0)
    col = lax.broadcasted_iota(jnp.int32, (8, LANES), 1)
    acc = jnp.zeros((8, LANES), jnp.float32)
    for s in range(3 * SLEVELS + 1):
        part = jnp.sum(jnp.where(bands == s, total, 0.0))
        acc = acc + jnp.where((row == time_band) & (col == s), part, 0.0)
    return acc


def panels_of(ref, width):
    def own(r, m):
        return [ref[r:r + m, p * LANES:(p + 1) * LANES] for p in range(width // LANES)]
    return own


def put_strip(one, at, strip, out_plane, sem):
    return [
        pltpu.make_async_copy(
            one.at[p, pl.ds(at, strip)], out_plane.at[:, p * LANES:(p + 1) * LANES], sem.at[p]
        )
        for p in range(one.shape[0])
    ]


def time_kernel(
    foot, blocks_ref, basis_ref, counts_ref, out, energy_ref,
    f, recv, g, o1, o3, s0, h, d2, t0, top, border, summary, shared, w_ref, one, two, three,
    in_sem, border_sem, send_sem, recv_sem, across, out_sem, sum_send, sum_recv,
):
    strip, width = foot.shape[1:]
    me, upper = lax.axis_index("frame"), lax.axis_index("row")
    devices = lax.axis_size("frame")
    left, right = lax.rem(me + devices - 1, devices), lax.rem(me + 1, devices)
    first, last = me == 0, me == devices - 1
    odd = lax.rem(me, 2) == 1
    size = strip // CHUNKS

    def rows(c):
        if isinstance(c, int) and c == CHUNKS:
            return pl.ds(strip, EXTRA)
        return pl.ds(pl.multiple_of(c * size, size), size)

    def send(level, side, c, src):
        return pltpu.make_async_remote_copy(
            src_ref=src.at[rows(c)],
            dst_ref=recv.at[level, side, rows(c)],
            send_sem=send_sem.at[level, side, c],
            recv_sem=recv_sem.at[level, side, c],
            device_id=(left if side == 0 else right, upper),
            device_id_type=pl.DeviceIdType.MESH,
        )

    def each(body, begin=0, end=CHUNKS):
        def step(c, carry):
            body(c)
            return carry
        lax.fori_loop(begin, end, step, 0)

    ring = 2 * Y_CHIPS
    x_at, z_at, y_at = me // (2 * ring), lax.rem(me // ring, 2), lax.rem(me, ring)
    base = me - y_at
    groups = (
        (y_at, [(base + k, upper) for k in range(ring)]),
        (
            x_at * 4 + z_at + 2 * upper,
            [(me + (k // 4 - x_at) * 2 * ring + (k % 2 - z_at) * ring, k // 2 % 2) for k in range(4 * (devices // (2 * ring)))],
        ),
    )

    barrier = pltpu.get_barrier_semaphore()

    def greet(where):
        pl.semaphore_signal(barrier, inc=1, device_id=where, device_id_type=pl.DeviceIdType.MESH)

    border_at = pl.multiple_of((strip - HALO) * (1 - upper), HALO)
    borders = pltpu.make_async_copy(foot.at[:, pl.ds(border_at, HALO)], border, border_sem)
    borders.start()
    loads = [pltpu.make_async_copy(foot.at[n], f.at[n, pl.ds(0, strip)], in_sem.at[n]) for n in range(4)]
    for n in (3, 2, 0, 1):
        loads[n].start()
    for slot, members in groups[::-1]:
        for k, where in enumerate(members):
            pl.when(slot != k)(functools.partial(greet, where))
    for where in ((left, upper), (right, upper)):
        greet(where)

    def partial(c):
        r = rows(c)
        g[r] = f[3, r] - 0.5 * f[2, r]

    def first_high(c):
        r = rows(c)
        o1[r] = f[1, r] - 0.5 * (f[0, r] + f[2, r])

    borders.wait()
    for n in range(4):
        values = border[n]
        for k in range(RANK):
            summary[n, k:k + 1, :] = (basis_ref[upper, :, k:k + 1] * values).sum(axis=0, keepdims=True)
        f[n, strip + RANK:, :] = jnp.zeros((EXTRA - RANK, width), jnp.float32)
    exchange = pltpu.make_async_remote_copy(
        src_ref=summary.at[:, pl.ds(0, RANK)],
        dst_ref=f.at[:, pl.ds(strip, RANK)],
        send_sem=across.at[0],
        recv_sem=across.at[1],
        device_id=(me, 1 - upper),
        device_id_type=pl.DeviceIdType.MESH,
    )
    loads[3].wait()
    loads[2].wait()
    each(partial)
    pl.semaphore_wait(barrier, 2 + sum(len(members) - 1 for _, members in groups))
    exchange.start()

    def first_left():
        each(lambda c: send(0, 0, c, foot.at[0]).start())

    def first_right():
        each(lambda c: send(0, 1, c, g).start())

    pl.when(y_at != 0)(first_left)
    pl.when(y_at != ring - 1)(first_right)
    loads[0].wait()
    loads[1].wait()
    each(first_high)
    exchange.wait_recv()
    pl.when(y_at == 0)(first_left)
    pl.when(y_at == ring - 1)(first_right)
    partial(CHUNKS)
    first_high(CHUNKS)
    send(0, 0, CHUNKS, f.at[0]).start()
    send(0, 1, CHUNKS, g).start()
    build_weights(blocks_ref, w_ref)
    bufs = (one, two, three)

    def halo_of(src):
        values = src[rows(CHUNKS)]
        total = basis_ref[1 - upper, :, 0:1] * values[0:1]
        for k in range(1, RANK):
            total = total + basis_ref[1 - upper, :, k:k + 1] * values[k:k + 1]
        return [total[:, p * LANES:(p + 1) * LANES] for p in range(width // LANES)]

    def plane_out(src, frame, time_band, previous):
        for copy in previous:
            copy.wait()
        first_columns(panels_of(src, width), lambda: halo_of(src), upper, w_ref, one)
        return rest_out(frame, time_band)

    def rest_out(frame, time_band):
        after_first_columns(w_ref, bufs)
        own_at = strip_rows(one, upper)[1]
        copies = put_strip(one, own_at, strip, out.at[frame], out_sem)
        for copy in copies:
            copy.start()
        return copies, band_energy(one, own_at, strip, time_band)

    def second(c):
        r = rows(c)
        send(0, 0, c, g).wait_recv()
        send(0, 1, c, g).wait_recv()
        f0, f2, first_o = f[0, r], f[2, r], o1[r]
        o_next = g[r] - 0.5 * jnp.where(last, f2, recv[0, 0, r])
        o_prev = jnp.where(first, first_o, recv[0, 1, r] - 0.5 * f0)
        low = f0 + 0.25 * (o_prev + first_o)
        o3[r] = o_next
        s0[r] = low
        h[r] = f2 + 0.25 * (first_o + o_next) - 0.5 * low
        send(1, 0, c, s0).start()
        send(1, 1, c, h).start()

    def third(c):
        r = rows(c)
        send(1, 0, c, s0).wait_recv()
        send(1, 1, c, h).wait_recv()
        low = s0[r]
        high = h[r] - 0.5 * jnp.where(last, low, recv[1, 0, r])
        high_prev = jnp.where(first, high, recv[1, 1, r] - 0.5 * low)
        d2[r] = high
        t = low + 0.25 * (high_prev + high)

        @pl.when(jnp.logical_not(odd))
        def _():
            t0[r] = t
            send(2, 1, c, t0).start()
            send(2, 0, c, t0).start()

        @pl.when(odd)
        def _():
            send(2, 1, c, t0).wait_recv()
            t0[r] = t - 0.5 * recv[2, 1, r]
            send(2, 1, c, t0).start()

    def fourth(c):
        r = rows(c)
        send(2, 0, c, t0).wait_recv()

        @pl.when(odd)
        def _():
            top[r] = t0[r] - 0.5 * jnp.where(last, recv[2, 1, r], recv[2, 0, r])
            send(2, 0, c, top).start()

        @pl.when(jnp.logical_not(odd))
        def _():
            send(2, 1, c, t0).wait_recv()
            mine, after = t0[r], recv[2, 0, r]
            prev = jnp.where(first, after, recv[2, 1, r] - 0.5 * mine)
            top[r] = mine + 0.25 * (prev + after)

    copies, energy1 = plane_out(o1, 1, 0, [])
    each(second)
    second(CHUNKS)
    copies, energy3 = plane_out(o3, 3, 0, copies)
    each(third)
    third(CHUNKS)
    copies, energy2 = plane_out(d2, 2, 1, copies)
    for copy in copies:
        copy.wait()
    own_at, halo_at = strip_rows(one, upper)[1:]

    def panels_at(r):
        return [top[r, p * LANES:(p + 1) * LANES] for p in range(width // LANES)]

    def finish(c):
        fourth(c)

        def store(p, value):
            one[p, pl.ds(pl.multiple_of(own_at + c * size, 8), size), :] = value

        columns(panels_at(rows(c)), w_ref, 0, store)

    each(finish, 0, CHUNKS - 1)
    fourth(CHUNKS - 1)
    fourth(CHUNKS)

    def store(p, value):
        one[p, pl.ds(pl.multiple_of(own_at + strip - size, 8), size), :] = value[:size]
        one[p, pl.ds(halo_at, HALO), :] = value[size:]

    ends = [jnp.concatenate(pair, axis=0) for pair in zip(panels_at(rows(CHUNKS - 1)), halo_of(top))]
    columns(ends, w_ref, 0, store)
    copies, energy0 = rest_out(0, jnp.where(odd, 2, 3))
    total = energy0 + energy1 + energy2 + energy3

    def tell(stage, k):
        slot, members = groups[stage]
        return pltpu.make_async_remote_copy(
            src_ref=shared.at[stage, slot],
            dst_ref=shared.at[stage, slot],
            send_sem=sum_send.at[stage, k],
            recv_sem=sum_recv.at[stage, slot],
            device_id=members[k],
            device_id_type=pl.DeviceIdType.MESH,
        )

    def heard(stage, k):
        return pltpu.make_async_remote_copy(
            src_ref=shared.at[stage, k],
            dst_ref=shared.at[stage, k],
            send_sem=sum_send.at[stage, k],
            recv_sem=sum_recv.at[stage, k],
            device_id=groups[stage][1][k],
            device_id_type=pl.DeviceIdType.MESH,
        )

    for stage, (slot, members) in enumerate(groups):
        shared[stage, slot] = total
        for k in range(len(members)):
            pl.when(slot != k)(lambda stage=stage, k=k: tell(stage, k).start())
        for k in range(len(members)):
            pl.when(slot != k)(lambda stage=stage, k=k: heard(stage, k).wait_recv())
        total = functools.reduce(jnp.add, [shared[stage, k] for k in range(len(members))])
    energy_ref[...] = total[:TLEVELS + 1, :3 * SLEVELS + 1] / counts_ref[...]

    for stage, (slot, members) in enumerate(groups):
        for k in range(len(members)):
            pl.when(slot != k)(lambda stage=stage, k=k: tell(stage, k).wait_send())
    for copy in copies:
        copy.wait()
    exchange.wait_send()

    def drain(c):
        send(0, 0, c, g).wait_send()
        send(0, 1, c, g).wait_send()
        send(1, 0, c, s0).wait_send()
        send(1, 1, c, h).wait_send()
        send(2, 0, c, top).wait_send()
        send(2, 1, c, t0).wait_send()

    each(drain)
    drain(CHUNKS)


def copy_kernel(src, energy_in, out, energy_out, stage, small, sems, small_sems):
    parts = stage.shape[0]
    frames, strip = src.shape[:2]
    size = frames * strip // parts

    def ends(k):
        at = pl.ds(k * size % strip, size)
        take = pltpu.make_async_copy(src.at[k * size // strip, at], stage.at[k], sems.at[0, k])
        put = pltpu.make_async_copy(stage.at[k], out.at[k * size // strip, at], sems.at[1, k])
        return take, put

    copies = [ends(k) for k in range(parts)]
    copies.append((
        pltpu.make_async_copy(energy_in, small, small_sems.at[0]),
        pltpu.make_async_copy(small, energy_out, small_sems.at[1]),
    ))
    for take, _ in copies:
        take.start()
    for take, put in copies:
        take.wait()
        put.start()
    for _, put in copies:
        put.wait()


def spatial_scratch(strip, width):
    panels, rows = width // LANES, strip + HALO
    return [pltpu.VMEM((SLEVELS, 2, 3, 4 * LANES, 2 * LANES), jnp.bfloat16)] + [
        pltpu.VMEM((panels, rows // k + 2 * PAD, LANES), jnp.float32) for k in (1, 2, 4)
    ]


def shards(footage):
    frames, strip, width = footage.shape
    blocks = jnp.asarray(weight_blocks(width))
    plane = pltpu.VMEM((strip + EXTRA, width), jnp.float32)
    dma = pltpu.SemaphoreType.DMA
    full = jax.ShapeDtypeStruct(footage.shape, jnp.float32)
    hbm = pl.BlockSpec(memory_space=pl.ANY)
    vmem = pl.BlockSpec(memory_space=pltpu.VMEM)
    devices = lax.axis_size("frame")
    size = counts(frames * devices, strip * lax.axis_size("row"), width)
    coeffs, energies = pl.pallas_call(
        time_kernel,
        out_shape=(full, jax.ShapeDtypeStruct(size.shape, jnp.float32)),
        in_specs=[hbm, vmem, vmem, vmem],
        out_specs=(hbm, vmem),
        scratch_shapes=[
            pltpu.VMEM((frames, strip + EXTRA, width), jnp.float32),
            pltpu.VMEM((3, 2, strip + EXTRA, width), jnp.float32),
            *[plane] * 8,
            pltpu.VMEM((frames, HALO, width), jnp.float32),
            pltpu.VMEM((frames, EXTRA, width), jnp.float32),
            pltpu.VMEM((2, 4 * Y_CHIPS, 8, LANES), jnp.float32),
            *spatial_scratch(strip, width),
            dma((4,)),
            dma,
            dma((3, 2, CHUNKS + 1)),
            dma((3, 2, CHUNKS + 1)),
            dma((2,)),
            dma((width // LANES,)),
            dma((2, 4 * Y_CHIPS)),
            dma((2, 4 * Y_CHIPS)),
        ],
        compiler_params=pltpu.CompilerParams(
            collective_id=0, has_side_effects=True, vmem_limit_bytes=60 * 2**20
        ),
        name="time",
    )(footage, blocks, jnp.asarray(summaries()), jnp.asarray(size, jnp.float32))
    parts = 16
    return pl.pallas_call(
        copy_kernel,
        out_shape=(full, jax.ShapeDtypeStruct(size.shape, jnp.float32)),
        in_specs=[hbm, hbm],
        out_specs=(hbm, hbm),
        scratch_shapes=[
            pltpu.VMEM((parts, frames * strip // parts, width), jnp.float32),
            pltpu.VMEM(size.shape, jnp.float32),
            dma((2, parts)),
            dma((2,)),
        ],
        compiler_params=pltpu.CompilerParams(vmem_limit_bytes=60 * 2**20),
        name="copy_out",
    )(coeffs, energies)


def solution(mesh):
    return jax.shard_map(
        shards,
        mesh=mesh,
        in_specs=(P("frame", "row", None),),
        out_specs=(P("frame", "row", None), P()),
        check_vma=False,
    )
```

```python
import functools

import jax
import jax.numpy as jnp
import ml_dtypes
import numpy as np
from jax import lax
from jax.experimental import pallas as pl
from jax.experimental.pallas import tpu as pltpu
from jax.sharding import PartitionSpec as P

SLEVELS = 3
TLEVELS = 3
ALPHA = -1.586134342
BETA = -0.05298011854
GAMMA = 0.8829110762
DELTA = 0.4435068522
ZETA = 1.149604398
HALO = 32
PAD = 8
LANES = 128
CHUNKS = 8
RANK = 2 * SLEVELS
EXTRA = 8
Y_CHIPS = 4


def lift_matrix(width):
    x = np.eye(width)
    e, o = x[:, 0::2], x[:, 1::2]
    after = lambda v: np.concatenate([v[:, 1:], v[:, -1:]], axis=1)
    before = lambda v: np.concatenate([v[:, :1], v[:, :-1]], axis=1)
    o = o + ALPHA * (e + after(e))
    e = e + BETA * (before(o) + o)
    o = o + GAMMA * (e + after(e))
    e = e + DELTA * (before(o) + o)
    out = np.zeros((width, width))
    out[:, 0::2] = e * ZETA
    out[:, 1::2] = o * (1.0 / ZETA)
    return out


def weight_blocks(width):
    levels = []
    for level in range(SLEVELS):
        s = 2**level
        m = np.zeros((width, width))
        m[::s, ::s] = lift_matrix(width // s)
        b = LANES
        mid = width // 2
        blocks = np.stack([
            m[:b, :b],
            m[mid:mid + b, mid:mid + b],
            m[width - b:, width - b:],
            m[mid - b:mid, mid:mid + b],
            m[mid + b:mid + 2 * b, mid:mid + b],
        ])
        hi = blocks.astype(ml_dtypes.bfloat16)
        lo = (blocks - hi.astype(np.float64)).astype(ml_dtypes.bfloat16)
        levels.append(np.stack([hi, lo]))
    return np.stack(levels)


TILES = (
    ((0, 3), (4, 1), (None, 4), (None, None)),
    ((3, None), (1, 3), (4, 1), (None, 4)),
    ((None, None), (3, None), (1, 3), (4, 2)),
)


def summaries():
    n = 4 * HALO
    steps, done = [], np.eye(n)
    for level in range(SLEVELS):
        s = 2**level
        step = np.eye(n)
        step[::s, ::s] = lift_matrix(n // s).T
        done = step @ done
        steps.append(done)
    half = n // 2
    result = np.zeros((2, HALO, LANES))
    for side, (mine, other) in enumerate(((slice(half, n), slice(half - HALO, half)), (slice(0, half), slice(half, half + HALO)))):
        cross = np.concatenate([m[mine, other] for m in steps])
        basis = np.linalg.svd(cross)[2][:RANK]
        result[side, :, :RANK] = basis.T
    return result.astype(np.float32)


def build_weights(blocks_ref, w_ref):
    zero = jnp.zeros((LANES, LANES), jnp.bfloat16)

    def fill(index, carry):
        level, part = index // 2, index % 2
        for kind in range(3):
            for r in range(4):
                for c in range(2):
                    which = TILES[kind][r][c]
                    value = zero if which is None else blocks_ref[level, part, which]
                    w_ref[level, part, kind, r * LANES:(r + 1) * LANES, c * LANES:(c + 1) * LANES] = value
        return carry

    lax.fori_loop(0, SLEVELS * 2, fill, 0)


def columns(xs, w_ref, level, store):
    count = len(xs)
    his, los = [], []
    for x in xs:
        hi = x.astype(jnp.bfloat16)
        his.append(hi)
        los.append((x - hi.astype(jnp.float32)).astype(jnp.bfloat16))
    for tile in range(count // 2):
        if tile == 0:
            kind, start = 0, 0
        elif tile == count // 2 - 1:
            kind, start = 2, count - 4
        else:
            kind, start = 1, 2 * tile - 1
        hi = jnp.concatenate(his[start:start + 4], axis=1)
        lo = jnp.concatenate(los[start:start + 4], axis=1)
        whi = w_ref[level, 0, kind]
        wlo = w_ref[level, 1, kind]
        dot = functools.partial(jnp.dot, preferred_element_type=jnp.float32)
        acc = dot(hi, whi) + dot(lo, whi) + dot(hi, wlo)
        store(2 * tile, acc[:, :LANES])
        store(2 * tile + 1, acc[:, LANES:])


def lift_rows(buf, pairs):
    ev = pl.ds(PAD, pairs, stride=2)
    od = pl.ds(PAD + 1, pairs, stride=2)
    ev_next = pl.ds(PAD + 2, pairs, stride=2)
    od_prev = pl.ds(PAD - 1, pairs, stride=2)
    end = PAD + 2 * pairs

    def panel(p, carry):
        def mirror_end():
            buf[p, end:end + 1, :] = buf[p, end - 2:end - 1, :]

        def mirror_start():
            buf[p, PAD - 1:PAD, :] = buf[p, PAD + 1:PAD + 2, :]

        mirror_end()
        buf[p, od, :] = buf[p, od, :] * (1.0 / ZETA) + (ALPHA / ZETA) * (buf[p, ev, :] + buf[p, ev_next, :])
        mirror_start()
        buf[p, ev, :] = buf[p, ev, :] + (BETA * ZETA) * (buf[p, od_prev, :] + buf[p, od, :])
        mirror_end()
        buf[p, od, :] = buf[p, od, :] + (GAMMA / ZETA) * (buf[p, ev, :] + buf[p, ev_next, :])
        mirror_start()
        buf[p, ev, :] = buf[p, ev, :] * ZETA + (DELTA * ZETA * ZETA) * (buf[p, od_prev, :] + buf[p, od, :])
        return carry

    lax.fori_loop(0, buf.shape[0], panel, 0, unroll=2)


def strip_rows(one, upper):
    strip = one.shape[1] - 2 * PAD - HALO
    own_at = pl.multiple_of(PAD + HALO * upper, 8)
    halo_at = pl.multiple_of(PAD + strip * (1 - upper), 8)
    return strip, own_at, halo_at


def first_columns(own, halo, upper, w_ref, one):
    strip, own_at, halo_at = strip_rows(one, upper)
    half = strip // 2

    def store_top(p, value):
        one[p, pl.ds(own_at, half), :] = value

    def store_rest(p, value):
        one[p, pl.ds(pl.multiple_of(own_at + half, 8), half), :] = value[:half]
        one[p, pl.ds(halo_at, HALO), :] = value[half:]

    columns(own(0, half), w_ref, 0, store_top)
    rest = [jnp.concatenate(pair, axis=0) for pair in zip(own(half, half), halo())]
    columns(rest, w_ref, 0, store_rest)


def after_first_columns(w_ref, bufs):
    one, two, three = bufs
    panels = one.shape[0]
    rows = one.shape[1] - 2 * PAD
    lift_rows(one, rows // 2)

    def into(buf, n):
        def store(p, value):
            buf[p, PAD:PAD + n, :] = value
        return store

    def evens(buf, n):
        return [buf[p, pl.ds(PAD, n, stride=2), :] for p in range(panels)]

    columns(evens(one, rows // 2), w_ref, 1, into(two, rows // 2))
    lift_rows(two, rows // 4)
    columns(evens(two, rows // 4), w_ref, 2, into(three, rows // 4))
    lift_rows(three, rows // 8)

    def merge(p, carry):
        lane = lax.broadcasted_iota(jnp.int32, (1, LANES), 1)
        n = rows // 4
        old = two[p, pl.ds(PAD, n, stride=2), :]
        two[p, pl.ds(PAD, n, stride=2), :] = jnp.where(lane % 4 == 0, three[p, PAD:PAD + n, :], old)
        n = rows // 2
        old = one[p, pl.ds(PAD, n, stride=2), :]
        one[p, pl.ds(PAD, n, stride=2), :] = jnp.where(lane % 2 == 0, two[p, PAD:PAD + n, :], old)
        return carry

    lax.fori_loop(0, panels, merge, 0, unroll=2)


def level_of(number, ceiling):
    depth = 1
    while number % 2 == 0 and depth <= ceiling:
        number //= 2
        depth += 1
    return depth


def band_of(row, col):
    u, v = level_of(row, SLEVELS), level_of(col, SLEVELS)
    m = min(u, v)
    if m > SLEVELS:
        return 3 * SLEVELS
    if u == v:
        return 3 * (m - 1) + 2
    return 3 * (m - 1) + (0 if u == m else 1)


def position_level(pos):
    return jnp.where(pos % 2 == 1, 1, jnp.where(pos % 4 == 2, 2, jnp.where(pos % 8 == 4, 3, 4)))


def band_table(shape):
    u = position_level(lax.broadcasted_iota(jnp.int32, shape, 0))
    v = position_level(lax.broadcasted_iota(jnp.int32, shape, 1))
    m = jnp.minimum(u, v)
    kind = jnp.where(u == v, 2, jnp.where(u == m, 0, 1))
    return jnp.where(m == SLEVELS + 1, 3 * SLEVELS, 3 * (m - 1) + kind)


def counts(frames, rows, cols):
    table = np.zeros(3 * SLEVELS + 1)
    for i in range(8):
        for j in range(8):
            table[band_of(i, j)] += 1 / 64
    share = np.array([0.5, 0.25, 0.125, 0.125])
    return float(frames) * rows * cols * np.outer(share, table)


def square_rows(one, at, n):
    def panel(p, acc):
        value = one[p, pl.ds(at, n), :]
        return acc + (value * value).reshape(-1, 8, LANES).sum(axis=0)

    return lax.fori_loop(0, one.shape[0], panel, jnp.zeros((8, LANES), jnp.float32), unroll=2)


def band_energy(total, time_band):
    bands = band_table((8, LANES))
    row = lax.broadcasted_iota(jnp.int32, (8, LANES), 0)
    col = lax.broadcasted_iota(jnp.int32, (8, LANES), 1)
    acc = jnp.zeros((8, LANES), jnp.float32)
    for s in range(3 * SLEVELS + 1):
        part = jnp.sum(jnp.where(bands == s, total, 0.0), axis=1, keepdims=True).sum(axis=0, keepdims=True)
        acc = acc + jnp.where((row == time_band) & (col == s), part, 0.0)
    return acc


def panels_of(ref, width):
    def own(r, m):
        return [ref[r:r + m, p * LANES:(p + 1) * LANES] for p in range(width // LANES)]
    return own


def put_rows(one, at, n, out_plane, to, sem):
    return [
        pltpu.make_async_copy(
            one.at[p, pl.ds(at, n)], out_plane.at[pl.ds(to, n), p * LANES:(p + 1) * LANES], sem.at[p]
        )
        for p in range(one.shape[0])
    ]


def time_kernel(
    foot, blocks_ref, basis_ref, counts_ref, out, energy_ref,
    f, recv, g, o1, o3, s0, h, d2, t0, top, border, summary, shared, w_ref, *rest,
):
    bufs, far_bufs, near_bufs = rest[0:3], rest[3:6], rest[6:9]
    one = bufs[0]
    in_sem, border_sem, send_sem, recv_sem, across, out_sem, sum_send, sum_recv = rest[9:]
    strip, width = foot.shape[1:]
    me, upper = lax.axis_index("frame"), lax.axis_index("row")
    devices = lax.axis_size("frame")
    left, right = lax.rem(me + devices - 1, devices), lax.rem(me + 1, devices)
    first, last = me == 0, me == devices - 1
    odd = lax.rem(me, 2) == 1
    size = strip // CHUNKS

    def rows(c):
        if isinstance(c, int) and c == CHUNKS:
            return pl.ds(strip, EXTRA)
        at = jnp.where(upper == 0, c, CHUNKS - 1 - c) * size
        return pl.ds(pl.multiple_of(at, size), size)

    def send(level, side, c, src):
        return pltpu.make_async_remote_copy(
            src_ref=src.at[rows(c)],
            dst_ref=recv.at[level, side, rows(c)],
            send_sem=send_sem.at[level, side, c],
            recv_sem=recv_sem.at[level, side, c],
            device_id=(left if side == 0 else right, upper),
            device_id_type=pl.DeviceIdType.MESH,
        )

    def each(body, begin=0, end=CHUNKS):
        def step(c, carry):
            body(c)
            return carry
        lax.fori_loop(begin, end, step, 0)

    ring = 2 * Y_CHIPS
    x_at, z_at, y_at = me // (2 * ring), lax.rem(me // ring, 2), lax.rem(me, ring)
    base = me - y_at
    groups = (
        (y_at, [(base + k, upper) for k in range(ring)]),
        (
            x_at * 4 + z_at + 2 * upper,
            [(me + (k // 4 - x_at) * 2 * ring + (k % 2 - z_at) * ring, k // 2 % 2) for k in range(4 * (devices // (2 * ring)))],
        ),
    )

    barrier = pltpu.get_barrier_semaphore()

    def greet(where):
        pl.semaphore_signal(barrier, inc=1, device_id=where, device_id_type=pl.DeviceIdType.MESH)

    border_at = pl.multiple_of((strip - HALO) * (1 - upper), HALO)
    borders = pltpu.make_async_copy(foot.at[:, pl.ds(border_at, HALO)], border, border_sem)
    borders.start()
    loads = [pltpu.make_async_copy(foot.at[n], f.at[n, pl.ds(0, strip)], in_sem.at[n]) for n in range(4)]
    for n in (3, 2, 0, 1):
        loads[n].start()
    for slot, members in groups[::-1]:
        for k, where in enumerate(members):
            pl.when(slot != k)(functools.partial(greet, where))
    for where in ((left, upper), (right, upper)):
        greet(where)

    def partial(c):
        r = rows(c)
        g[r] = f[3, r] - 0.5 * f[2, r]

    def first_high(c):
        r = rows(c)
        o1[r] = f[1, r] - 0.5 * (f[0, r] + f[2, r])

    borders.wait()
    for n in range(4):
        values = border[n]
        for k in range(RANK):
            summary[n, k:k + 1, :] = (basis_ref[upper, :, k:k + 1] * values).sum(axis=0, keepdims=True)
        f[n, strip + RANK:, :] = jnp.zeros((EXTRA - RANK, width), jnp.float32)
    exchange = pltpu.make_async_remote_copy(
        src_ref=summary.at[:, pl.ds(0, RANK)],
        dst_ref=f.at[:, pl.ds(strip, RANK)],
        send_sem=across.at[0],
        recv_sem=across.at[1],
        device_id=(me, 1 - upper),
        device_id_type=pl.DeviceIdType.MESH,
    )
    loads[3].wait()
    loads[2].wait()
    each(partial)
    pl.semaphore_wait(barrier, 2 + sum(len(members) - 1 for _, members in groups))
    exchange.start()

    def first_left():
        each(lambda c: send(0, 0, c, foot.at[0]).start())

    def first_right():
        each(lambda c: send(0, 1, c, g).start())

    pl.when(y_at != 0)(first_left)
    pl.when(y_at != ring - 1)(first_right)
    loads[0].wait()
    loads[1].wait()
    each(first_high)
    exchange.wait_recv()
    pl.when(y_at == 0)(first_left)
    pl.when(y_at == ring - 1)(first_right)
    partial(CHUNKS)
    first_high(CHUNKS)
    send(0, 0, CHUNKS, f.at[0]).start()
    send(0, 1, CHUNKS, g).start()
    build_weights(blocks_ref, w_ref)
    def halo_of(src):
        values = src[rows(CHUNKS)]
        total = basis_ref[1 - upper, :, 0:1] * values[0:1]
        for k in range(1, RANK):
            total = total + basis_ref[1 - upper, :, k:k + 1] * values[k:k + 1]
        return [total[:, p * LANES:(p + 1) * LANES] for p in range(width // LANES)]

    def plane_out(src, frame, time_band, previous):
        for copy in previous:
            copy.wait()
        first_columns(panels_of(src, width), lambda: halo_of(src), upper, w_ref, one)
        after_first_columns(w_ref, bufs)
        own_at = strip_rows(one, upper)[1]
        copies = put_rows(one, own_at, strip, out.at[frame], 0, out_sem.at[0])
        for copy in copies:
            copy.start()
        return copies, band_energy(square_rows(one, own_at, strip), time_band)

    def second(c):
        r = rows(c)
        send(0, 0, c, g).wait_recv()
        send(0, 1, c, g).wait_recv()
        f0, f2, first_o = f[0, r], f[2, r], o1[r]
        o_next = g[r] - 0.5 * jnp.where(last, f2, recv[0, 0, r])
        o_prev = jnp.where(first, first_o, recv[0, 1, r] - 0.5 * f0)
        low = f0 + 0.25 * (o_prev + first_o)
        o3[r] = o_next
        s0[r] = low
        h[r] = f2 + 0.25 * (first_o + o_next) - 0.5 * low
        send(1, 0, c, s0).start()
        send(1, 1, c, h).start()

    def third(c):
        r = rows(c)
        send(1, 0, c, s0).wait_recv()
        send(1, 1, c, h).wait_recv()
        low = s0[r]
        high = h[r] - 0.5 * jnp.where(last, low, recv[1, 0, r])
        high_prev = jnp.where(first, high, recv[1, 1, r] - 0.5 * low)
        d2[r] = high
        t = low + 0.25 * (high_prev + high)

        @pl.when(jnp.logical_not(odd))
        def _():
            t0[r] = t
            send(2, 1, c, t0).start()
            send(2, 0, c, t0).start()

        @pl.when(odd)
        def _():
            send(2, 1, c, t0).wait_recv()
            t0[r] = t - 0.5 * recv[2, 1, r]
            send(2, 1, c, t0).start()

    def fourth(c):
        r = rows(c)
        send(2, 0, c, t0).wait_recv()

        @pl.when(odd)
        def _():
            top[r] = t0[r] - 0.5 * jnp.where(last, recv[2, 1, r], recv[2, 0, r])
            send(2, 0, c, top).start()

        @pl.when(jnp.logical_not(odd))
        def _():
            send(2, 1, c, t0).wait_recv()
            mine, after = t0[r], recv[2, 0, r]
            prev = jnp.where(first, after, recv[2, 1, r] - 0.5 * mine)
            top[r] = mine + 0.25 * (prev + after)

    copies, energy1 = plane_out(o1, 1, 0, [])
    each(second)
    second(CHUNKS)
    copies, energy3 = plane_out(o3, 3, 0, copies)
    each(third)
    third(CHUNKS)
    copies, energy2 = plane_out(d2, 2, 1, copies)

    far = CHUNKS - 2
    far_base = (strip - far * size) * upper
    near_shift = jnp.where(upper == 0, -(far - 1) * size, HALO)
    near_halo = 3 * size * (1 - upper)

    def into(buf, at, n):
        return buf, pl.ds(pl.multiple_of(PAD + at, 8), n)

    def finish(c, targets, halo=None):
        values = [top[rows(c), p * LANES:(p + 1) * LANES] for p in range(width // LANES)]
        if halo is not None:
            values = [jnp.concatenate(pair, axis=0) for pair in zip(values, halo)]

        def store(p, value):
            for (buf, r), begin in targets:
                buf[p, r, :] = value[begin:begin + r.size]

        columns(values, w_ref, 0, store)

    def finish_far(c):
        fourth(c)
        finish(c, [(into(far_bufs[0], rows(c).start - far_base, size), 0)])

    each(finish_far, 0, far - 1)
    at = rows(far - 1).start
    fourth(far - 1)
    finish(far - 1, [(into(far_bufs[0], at - far_base, size), 0), (into(near_bufs[0], at + near_shift, size), 0)])
    after_first_columns(w_ref, far_bufs)
    far_rows = far * size - HALO
    far_at = pl.multiple_of(PAD + HALO * upper, 8)
    far_to = pl.multiple_of((strip - far_rows) * upper, 8)
    far_copies = put_rows(far_bufs[0], far_at, far_rows, out.at[0], far_to, out_sem.at[1])
    for copy in far_copies:
        copy.start()
    squares = square_rows(far_bufs[0], far_at, far_rows)

    fourth(CHUNKS - 2)
    finish(CHUNKS - 2, [(into(near_bufs[0], rows(CHUNKS - 2).start + near_shift, size), 0)])
    fourth(CHUNKS - 1)
    fourth(CHUNKS)
    near_last = into(near_bufs[0], rows(CHUNKS - 1).start + near_shift, size)
    finish(CHUNKS - 1, [(near_last, 0), (into(near_bufs[0], near_halo, HALO), size)], halo_of(top))
    after_first_columns(w_ref, near_bufs)
    near_rows = strip - far_rows
    near_to = pl.multiple_of(far_rows * (1 - upper), 8)
    near_copies = put_rows(near_bufs[0], PAD + HALO, near_rows, out.at[0], near_to, out_sem.at[2])
    for copy in near_copies:
        copy.start()
    squares = squares + square_rows(near_bufs[0], PAD + HALO, near_rows)
    copies = copies + far_copies + near_copies
    energy0 = band_energy(squares, jnp.where(odd, 2, 3))
    total = energy0 + energy1 + energy2 + energy3

    def tell(stage, k):
        slot, members = groups[stage]
        return pltpu.make_async_remote_copy(
            src_ref=shared.at[stage, slot],
            dst_ref=shared.at[stage, slot],
            send_sem=sum_send.at[stage, k],
            recv_sem=sum_recv.at[stage, slot],
            device_id=members[k],
            device_id_type=pl.DeviceIdType.MESH,
        )

    def heard(stage, k):
        return pltpu.make_async_remote_copy(
            src_ref=shared.at[stage, k],
            dst_ref=shared.at[stage, k],
            send_sem=sum_send.at[stage, k],
            recv_sem=sum_recv.at[stage, k],
            device_id=groups[stage][1][k],
            device_id_type=pl.DeviceIdType.MESH,
        )

    for stage, (slot, members) in enumerate(groups):
        shared[stage, slot] = total
        for k in range(len(members)):
            pl.when(slot != k)(lambda stage=stage, k=k: tell(stage, k).start())
        for k in range(len(members)):
            pl.when(slot != k)(lambda stage=stage, k=k: heard(stage, k).wait_recv())
        total = functools.reduce(jnp.add, [shared[stage, k] for k in range(len(members))])
    energy_ref[...] = total[:TLEVELS + 1, :3 * SLEVELS + 1] / counts_ref[...]

    for stage, (slot, members) in enumerate(groups):
        for k in range(len(members)):
            pl.when(slot != k)(lambda stage=stage, k=k: tell(stage, k).wait_send())
    for copy in copies:
        copy.wait()
    exchange.wait_send()

    def drain(c):
        send(0, 0, c, g).wait_send()
        send(0, 1, c, g).wait_send()
        send(1, 0, c, s0).wait_send()
        send(1, 1, c, h).wait_send()
        send(2, 0, c, top).wait_send()
        send(2, 1, c, t0).wait_send()

    each(drain)
    drain(CHUNKS)


def copy_kernel(src, energy_in, out, energy_out, stage, small, sems, small_sems):
    parts = stage.shape[0]
    frames, strip = src.shape[:2]
    size = frames * strip // parts

    def ends(k):
        at = pl.ds(k * size % strip, size)
        take = pltpu.make_async_copy(src.at[k * size // strip, at], stage.at[k], sems.at[0, k])
        put = pltpu.make_async_copy(stage.at[k], out.at[k * size // strip, at], sems.at[1, k])
        return take, put

    copies = [ends(k) for k in range(parts)]
    copies.append((
        pltpu.make_async_copy(energy_in, small, small_sems.at[0]),
        pltpu.make_async_copy(small, energy_out, small_sems.at[1]),
    ))
    for take, _ in copies:
        take.start()
    for take, put in copies:
        take.wait()
        put.start()
    for _, put in copies:
        put.wait()


def row_buffers(rows, width):
    return [pltpu.VMEM((width // LANES, rows // k + 2 * PAD, LANES), jnp.float32) for k in (1, 2, 4)]


def shards(footage):
    frames, strip, width = footage.shape
    blocks = jnp.asarray(weight_blocks(width))
    plane = pltpu.VMEM((strip + EXTRA, width), jnp.float32)
    dma = pltpu.SemaphoreType.DMA
    full = jax.ShapeDtypeStruct(footage.shape, jnp.float32)
    hbm = pl.BlockSpec(memory_space=pl.ANY)
    vmem = pl.BlockSpec(memory_space=pltpu.VMEM)
    devices = lax.axis_size("frame")
    size = counts(frames * devices, strip * lax.axis_size("row"), width)
    coeffs, energies = pl.pallas_call(
        time_kernel,
        out_shape=(full, jax.ShapeDtypeStruct(size.shape, jnp.float32)),
        in_specs=[hbm, vmem, vmem, vmem],
        out_specs=(hbm, vmem),
        scratch_shapes=[
            pltpu.VMEM((frames, strip + EXTRA, width), jnp.float32),
            pltpu.VMEM((3, 2, strip + EXTRA, width), jnp.float32),
            *[plane] * 8,
            pltpu.VMEM((frames, HALO, width), jnp.float32),
            pltpu.VMEM((frames, EXTRA, width), jnp.float32),
            pltpu.VMEM((2, 4 * Y_CHIPS, 8, LANES), jnp.float32),
            pltpu.VMEM((SLEVELS, 2, 3, 4 * LANES, 2 * LANES), jnp.bfloat16),
            *row_buffers(strip + HALO, width),
            *row_buffers((CHUNKS - 2) * (strip // CHUNKS), width),
            *row_buffers(3 * (strip // CHUNKS) + HALO, width),
            dma((4,)),
            dma,
            dma((3, 2, CHUNKS + 1)),
            dma((3, 2, CHUNKS + 1)),
            dma((2,)),
            dma((3, width // LANES)),
            dma((2, 4 * Y_CHIPS)),
            dma((2, 4 * Y_CHIPS)),
        ],
        compiler_params=pltpu.CompilerParams(
            collective_id=0, has_side_effects=True, vmem_limit_bytes=60 * 2**20
        ),
        name="time",
    )(footage, blocks, jnp.asarray(summaries()), jnp.asarray(size, jnp.float32))
    parts = 16
    return pl.pallas_call(
        copy_kernel,
        out_shape=(full, jax.ShapeDtypeStruct(size.shape, jnp.float32)),
        in_specs=[hbm, hbm],
        out_specs=(hbm, hbm),
        scratch_shapes=[
            pltpu.VMEM((parts, frames * strip // parts, width), jnp.float32),
            pltpu.VMEM(size.shape, jnp.float32),
            dma((2, parts)),
            dma((2,)),
        ],
        compiler_params=pltpu.CompilerParams(vmem_limit_bytes=60 * 2**20),
        name="copy_out",
    )(coeffs, energies)


def solution(mesh):
    return jax.shard_map(
        shards,
        mesh=mesh,
        in_specs=(P("frame", "row", None),),
        out_specs=(P("frame", "row", None), P()),
        check_vma=False,
    )
```

```python
import functools

import jax
import jax.numpy as jnp
import ml_dtypes
import numpy as np
from jax import lax
from jax.experimental import pallas as pl
from jax.experimental.pallas import tpu as pltpu
from jax.sharding import PartitionSpec as P

SLEVELS = 3
TLEVELS = 3
ALPHA = -1.586134342
BETA = -0.05298011854
GAMMA = 0.8829110762
DELTA = 0.4435068522
ZETA = 1.149604398
HALO = 32
PAD = 8
LANES = 128
CHUNKS = 8
RANK = 2 * SLEVELS
EXTRA = 8
Y_CHIPS = 4


def lift_matrix(width):
    x = np.eye(width)
    e, o = x[:, 0::2], x[:, 1::2]
    after = lambda v: np.concatenate([v[:, 1:], v[:, -1:]], axis=1)
    before = lambda v: np.concatenate([v[:, :1], v[:, :-1]], axis=1)
    o = o + ALPHA * (e + after(e))
    e = e + BETA * (before(o) + o)
    o = o + GAMMA * (e + after(e))
    e = e + DELTA * (before(o) + o)
    out = np.zeros((width, width))
    out[:, 0::2] = e * ZETA
    out[:, 1::2] = o * (1.0 / ZETA)
    return out


def weight_blocks(width):
    levels = []
    for level in range(SLEVELS):
        s = 2**level
        m = np.zeros((width, width))
        m[::s, ::s] = lift_matrix(width // s)
        b = LANES
        mid = width // 2
        blocks = np.stack([
            m[:b, :b],
            m[mid:mid + b, mid:mid + b],
            m[width - b:, width - b:],
            m[mid - b:mid, mid:mid + b],
            m[mid + b:mid + 2 * b, mid:mid + b],
        ])
        hi = blocks.astype(ml_dtypes.bfloat16)
        lo = (blocks - hi.astype(np.float64)).astype(ml_dtypes.bfloat16)
        levels.append(np.stack([hi, lo]))
    return np.stack(levels)


TILES = (
    ((0, 3), (4, 1), (None, 4), (None, None)),
    ((3, None), (1, 3), (4, 1), (None, 4)),
    ((None, None), (3, None), (1, 3), (4, 2)),
)


def summaries():
    n = 4 * HALO
    steps, done = [], np.eye(n)
    for level in range(SLEVELS):
        s = 2**level
        step = np.eye(n)
        step[::s, ::s] = lift_matrix(n // s).T
        done = step @ done
        steps.append(done)
    half = n // 2
    result = np.zeros((2, HALO, LANES))
    for side, (mine, other) in enumerate(((slice(half, n), slice(half - HALO, half)), (slice(0, half), slice(half, half + HALO)))):
        cross = np.concatenate([m[mine, other] for m in steps])
        basis = np.linalg.svd(cross)[2][:RANK]
        result[side, :, :RANK] = basis.T
    return result.astype(np.float32)


def build_weights(blocks_ref, w_ref):
    zero = jnp.zeros((LANES, LANES), jnp.bfloat16)

    def fill(index, carry):
        level, part = index // 2, index % 2
        for kind in range(3):
            for r in range(4):
                for c in range(2):
                    which = TILES[kind][r][c]
                    value = zero if which is None else blocks_ref[level, part, which]
                    w_ref[level, part, kind, r * LANES:(r + 1) * LANES, c * LANES:(c + 1) * LANES] = value
        return carry

    lax.fori_loop(0, SLEVELS * 2, fill, 0)


def columns(xs, w_ref, level, store):
    count = len(xs)
    his, los = [], []
    for x in xs:
        hi = x.astype(jnp.bfloat16)
        his.append(hi)
        los.append((x - hi.astype(jnp.float32)).astype(jnp.bfloat16))
    for tile in range(count // 2):
        if tile == 0:
            kind, start = 0, 0
        elif tile == count // 2 - 1:
            kind, start = 2, count - 4
        else:
            kind, start = 1, 2 * tile - 1
        hi = jnp.concatenate(his[start:start + 4], axis=1)
        lo = jnp.concatenate(los[start:start + 4], axis=1)
        whi = w_ref[level, 0, kind]
        wlo = w_ref[level, 1, kind]
        dot = functools.partial(jnp.dot, preferred_element_type=jnp.float32)
        acc = dot(hi, whi) + dot(lo, whi) + dot(hi, wlo)
        store(2 * tile, acc[:, :LANES])
        store(2 * tile + 1, acc[:, LANES:])


def lift_rows(buf, pairs):
    ev = pl.ds(PAD, pairs, stride=2)
    od = pl.ds(PAD + 1, pairs, stride=2)
    ev_next = pl.ds(PAD + 2, pairs, stride=2)
    od_prev = pl.ds(PAD - 1, pairs, stride=2)
    end = PAD + 2 * pairs

    def panel(p, carry):
        def mirror_end():
            buf[p, end:end + 1, :] = buf[p, end - 2:end - 1, :]

        def mirror_start():
            buf[p, PAD - 1:PAD, :] = buf[p, PAD + 1:PAD + 2, :]

        mirror_end()
        buf[p, od, :] = buf[p, od, :] * (1.0 / ZETA) + (ALPHA / ZETA) * (buf[p, ev, :] + buf[p, ev_next, :])
        mirror_start()
        buf[p, ev, :] = buf[p, ev, :] + (BETA * ZETA) * (buf[p, od_prev, :] + buf[p, od, :])
        mirror_end()
        buf[p, od, :] = buf[p, od, :] + (GAMMA / ZETA) * (buf[p, ev, :] + buf[p, ev_next, :])
        mirror_start()
        buf[p, ev, :] = buf[p, ev, :] * ZETA + (DELTA * ZETA * ZETA) * (buf[p, od_prev, :] + buf[p, od, :])
        return carry

    lax.fori_loop(0, buf.shape[0], panel, 0, unroll=2)


def strip_rows(one, upper):
    strip = one.shape[1] - 3 * PAD - HALO
    own_at = pl.multiple_of(PAD + HALO * upper, 8)
    halo_at = pl.multiple_of(PAD + strip * (1 - upper), 8)
    return strip, own_at, halo_at


def first_columns(own, halo, upper, w_ref, one):
    strip, own_at, halo_at = strip_rows(one, upper)
    half = strip // 2

    def store_top(p, value):
        one[p, pl.ds(own_at, half), :] = value

    def store_rest(p, value):
        one[p, pl.ds(pl.multiple_of(own_at + half, 8), half), :] = value[:half]
        one[p, pl.ds(halo_at, HALO), :] = value[half:]

    columns(own(0, half), w_ref, 0, store_top)
    rest = [jnp.concatenate(pair, axis=0) for pair in zip(own(half, half), halo())]
    columns(rest, w_ref, 0, store_rest)


def after_first_columns(w_ref, bufs):
    one, two, three = bufs
    panels = one.shape[0]
    rows = one.shape[1] - 3 * PAD
    lift_rows(one, rows // 2)

    def into(buf, n):
        def store(p, value):
            buf[p, PAD:PAD + n, :] = value
        return store

    def evens(buf, n):
        return [buf[p, pl.ds(PAD, n, stride=2), :] for p in range(panels)]

    columns(evens(one, rows // 2), w_ref, 1, into(two, rows // 2))
    lift_rows(two, rows // 4)
    columns(evens(two, rows // 4), w_ref, 2, into(three, rows // 4))
    lift_rows(three, rows // 8)

    def merge(p, carry):
        lane = lax.broadcasted_iota(jnp.int32, (1, LANES), 1)
        n = rows // 4
        old = two[p, pl.ds(PAD, n, stride=2), :]
        two[p, pl.ds(PAD, n, stride=2), :] = jnp.where(lane % 4 == 0, three[p, PAD:PAD + n, :], old)
        n = rows // 2
        old = one[p, pl.ds(PAD, n, stride=2), :]
        one[p, pl.ds(PAD, n, stride=2), :] = jnp.where(lane % 2 == 0, two[p, PAD:PAD + n, :], old)
        return carry

    lax.fori_loop(0, panels, merge, 0, unroll=2)


def level_of(number, ceiling):
    depth = 1
    while number % 2 == 0 and depth <= ceiling:
        number //= 2
        depth += 1
    return depth


def band_of(row, col):
    u, v = level_of(row, SLEVELS), level_of(col, SLEVELS)
    m = min(u, v)
    if m > SLEVELS:
        return 3 * SLEVELS
    if u == v:
        return 3 * (m - 1) + 2
    return 3 * (m - 1) + (0 if u == m else 1)


def position_level(pos):
    return jnp.where(pos % 2 == 1, 1, jnp.where(pos % 4 == 2, 2, jnp.where(pos % 8 == 4, 3, 4)))


def band_table(shape):
    u = position_level(lax.broadcasted_iota(jnp.int32, shape, 0))
    v = position_level(lax.broadcasted_iota(jnp.int32, shape, 1))
    m = jnp.minimum(u, v)
    kind = jnp.where(u == v, 2, jnp.where(u == m, 0, 1))
    return jnp.where(m == SLEVELS + 1, 3 * SLEVELS, 3 * (m - 1) + kind)


def counts(frames, rows, cols):
    table = np.zeros(3 * SLEVELS + 1)
    for i in range(8):
        for j in range(8):
            table[band_of(i, j)] += 1 / 64
    share = np.array([0.5, 0.25, 0.125, 0.125])
    return float(frames) * rows * cols * np.outer(share, table)


def square_rows(one, at, n):
    def panel(p, acc):
        value = one[p, pl.ds(at, n), :]
        return acc + (value * value).reshape(-1, 8, LANES).sum(axis=0)

    return lax.fori_loop(0, one.shape[0], panel, jnp.zeros((8, LANES), jnp.float32), unroll=2)


def band_energy(total, time_band):
    bands = band_table((8, LANES))
    row = lax.broadcasted_iota(jnp.int32, (8, LANES), 0)
    col = lax.broadcasted_iota(jnp.int32, (8, LANES), 1)
    acc = jnp.zeros((8, LANES), jnp.float32)
    for s in range(3 * SLEVELS + 1):
        part = jnp.sum(jnp.where(bands == s, total, 0.0), axis=1, keepdims=True).sum(axis=0, keepdims=True)
        acc = acc + jnp.where((row == time_band) & (col == s), part, 0.0)
    return acc


def panels_of(ref, width):
    def own(r, m):
        return [ref[r:r + m, p * LANES:(p + 1) * LANES] for p in range(width // LANES)]
    return own


def put_rows(one, at, n, out_plane, to, sem):
    return [
        pltpu.make_async_copy(
            one.at[p, pl.ds(at, n)], out_plane.at[pl.ds(to, n), p * LANES:(p + 1) * LANES], sem.at[p]
        )
        for p in range(one.shape[0])
    ]


def time_kernel(
    foot, blocks_ref, basis_ref, counts_ref, out, energy_ref,
    f, recv, g, o1, o3, s0, h, d2, t0, top, border, summary, shared, w_ref, *rest,
):
    bufs, far_bufs, near_bufs = rest[0:3], rest[3:6], rest[6:9]
    one = bufs[0]
    in_sem, border_sem, send_sem, recv_sem, across, out_sem, sum_send, sum_recv = rest[9:]
    strip, width = foot.shape[1:]
    me, upper = lax.axis_index("frame"), lax.axis_index("row")
    devices = lax.axis_size("frame")
    left, right = lax.rem(me + devices - 1, devices), lax.rem(me + 1, devices)
    first, last = me == 0, me == devices - 1
    odd = lax.rem(me, 2) == 1
    size = strip // CHUNKS

    def rows(c):
        if isinstance(c, int) and c == CHUNKS:
            return pl.ds(strip, EXTRA)
        at = jnp.where(upper == 0, c, CHUNKS - 1 - c) * size
        return pl.ds(pl.multiple_of(at, size), size)

    def send(level, side, c, src):
        return pltpu.make_async_remote_copy(
            src_ref=src.at[rows(c)],
            dst_ref=recv.at[level, side, rows(c)],
            send_sem=send_sem.at[level, side, c],
            recv_sem=recv_sem.at[level, side, c],
            device_id=(left if side == 0 else right, upper),
            device_id_type=pl.DeviceIdType.MESH,
        )

    def each(body, begin=0, end=CHUNKS):
        def step(c, carry):
            body(c)
            return carry
        lax.fori_loop(begin, end, step, 0)

    ring = 2 * Y_CHIPS
    x_at, z_at, y_at = me // (2 * ring), lax.rem(me // ring, 2), lax.rem(me, ring)
    base = me - y_at
    groups = (
        (y_at, [(base + k, upper) for k in range(ring)]),
        (
            x_at * 4 + z_at + 2 * upper,
            [(me + (k // 4 - x_at) * 2 * ring + (k % 2 - z_at) * ring, k // 2 % 2) for k in range(4 * (devices // (2 * ring)))],
        ),
    )

    barrier = pltpu.get_barrier_semaphore()

    def greet(where):
        pl.semaphore_signal(barrier, inc=1, device_id=where, device_id_type=pl.DeviceIdType.MESH)

    border_at = pl.multiple_of((strip - HALO) * (1 - upper), HALO)
    borders = pltpu.make_async_copy(foot.at[:, pl.ds(border_at, HALO)], border, border_sem)
    borders.start()
    loads = [pltpu.make_async_copy(foot.at[n], f.at[n, pl.ds(0, strip)], in_sem.at[n]) for n in range(4)]
    for n in (3, 2, 0, 1):
        loads[n].start()
    for slot, members in groups[::-1]:
        for k, where in enumerate(members):
            pl.when(slot != k)(functools.partial(greet, where))
    for where in ((left, upper), (right, upper)):
        greet(where)

    def partial(c):
        r = rows(c)
        g[r] = f[3, r] - 0.5 * f[2, r]

    def first_high(c):
        r = rows(c)
        o1[r] = f[1, r] - 0.5 * (f[0, r] + f[2, r])

    borders.wait()
    for n in range(4):
        values = border[n]
        for k in range(RANK):
            summary[n, k:k + 1, :] = (basis_ref[upper, :, k:k + 1] * values).sum(axis=0, keepdims=True)
        f[n, strip + RANK:, :] = jnp.zeros((EXTRA - RANK, width), jnp.float32)
    exchange = pltpu.make_async_remote_copy(
        src_ref=summary.at[:, pl.ds(0, RANK)],
        dst_ref=f.at[:, pl.ds(strip, RANK)],
        send_sem=across.at[0],
        recv_sem=across.at[1],
        device_id=(me, 1 - upper),
        device_id_type=pl.DeviceIdType.MESH,
    )
    loads[3].wait()
    loads[2].wait()
    each(partial)
    pl.semaphore_wait(barrier, 2 + sum(len(members) - 1 for _, members in groups))
    exchange.start()

    def first_left():
        each(lambda c: send(0, 0, c, foot.at[0]).start())

    def first_right():
        each(lambda c: send(0, 1, c, g).start())

    pl.when(y_at != 0)(first_left)
    pl.when(y_at != ring - 1)(first_right)
    loads[0].wait()
    loads[1].wait()
    each(first_high)
    exchange.wait_recv()
    pl.when(y_at == 0)(first_left)
    pl.when(y_at == ring - 1)(first_right)
    partial(CHUNKS)
    first_high(CHUNKS)
    send(0, 0, CHUNKS, f.at[0]).start()
    send(0, 1, CHUNKS, g).start()
    build_weights(blocks_ref, w_ref)
    def halo_of(src):
        values = src[rows(CHUNKS)]
        total = basis_ref[1 - upper, :, 0:1] * values[0:1]
        for k in range(1, RANK):
            total = total + basis_ref[1 - upper, :, k:k + 1] * values[k:k + 1]
        return [total[:, p * LANES:(p + 1) * LANES] for p in range(width // LANES)]

    def plane_out(src, frame, time_band, previous):
        for copy in previous:
            copy.wait()
        first_columns(panels_of(src, width), lambda: halo_of(src), upper, w_ref, one)
        after_first_columns(w_ref, bufs)
        own_at = strip_rows(one, upper)[1]
        copies = put_rows(one, own_at, strip, out.at[frame], 0, out_sem.at[0])
        for copy in copies:
            copy.start()
        return copies, band_energy(square_rows(one, own_at, strip), time_band)

    def second(c):
        r = rows(c)
        send(0, 0, c, g).wait_recv()
        send(0, 1, c, g).wait_recv()
        f0, f2, first_o = f[0, r], f[2, r], o1[r]
        o_next = g[r] - 0.5 * jnp.where(last, f2, recv[0, 0, r])
        o_prev = jnp.where(first, first_o, recv[0, 1, r] - 0.5 * f0)
        low = f0 + 0.25 * (o_prev + first_o)
        o3[r] = o_next
        s0[r] = low
        h[r] = f2 + 0.25 * (first_o + o_next) - 0.5 * low
        send(1, 0, c, s0).start()
        send(1, 1, c, h).start()

    def third(c):
        r = rows(c)
        send(1, 0, c, s0).wait_recv()
        send(1, 1, c, h).wait_recv()
        low = s0[r]
        high = h[r] - 0.5 * jnp.where(last, low, recv[1, 0, r])
        high_prev = jnp.where(first, high, recv[1, 1, r] - 0.5 * low)
        d2[r] = high
        t = low + 0.25 * (high_prev + high)

        @pl.when(jnp.logical_not(odd))
        def _():
            t0[r] = t
            send(2, 1, c, t0).start()
            send(2, 0, c, t0).start()

        @pl.when(odd)
        def _():
            send(2, 1, c, t0).wait_recv()
            t0[r] = t - 0.5 * recv[2, 1, r]
            send(2, 1, c, t0).start()

    def fourth(c):
        r = rows(c)
        send(2, 0, c, t0).wait_recv()

        @pl.when(odd)
        def _():
            top[r] = t0[r] - 0.5 * jnp.where(last, recv[2, 1, r], recv[2, 0, r])
            send(2, 0, c, top).start()

        @pl.when(jnp.logical_not(odd))
        def _():
            send(2, 1, c, t0).wait_recv()
            mine, after = t0[r], recv[2, 0, r]
            prev = jnp.where(first, after, recv[2, 1, r] - 0.5 * mine)
            top[r] = mine + 0.25 * (prev + after)

    copies, energy1 = plane_out(o1, 1, 0, [])
    each(second)
    second(CHUNKS)
    copies, energy3 = plane_out(o3, 3, 0, copies)
    each(third)
    third(CHUNKS)
    copies, energy2 = plane_out(d2, 2, 1, copies)

    far = CHUNKS - 2
    far_base = (strip - far * size) * upper
    near_shift = jnp.where(upper == 0, -(far - 1) * size, HALO)
    near_halo = 3 * size * (1 - upper)

    def into(buf, at, n):
        return buf, pl.ds(pl.multiple_of(PAD + at, 8), n)

    def finish(c, targets, halo=None):
        values = [top[rows(c), p * LANES:(p + 1) * LANES] for p in range(width // LANES)]
        if halo is not None:
            values = [jnp.concatenate(pair, axis=0) for pair in zip(values, halo)]

        def store(p, value):
            for (buf, r), begin in targets:
                buf[p, r, :] = value[begin:begin + r.size]

        columns(values, w_ref, 0, store)

    def finish_far(c):
        fourth(c)
        finish(c, [(into(far_bufs[0], rows(c).start - far_base, size), 0)])

    each(finish_far, 0, far - 1)
    at = rows(far - 1).start
    fourth(far - 1)
    finish(far - 1, [(into(far_bufs[0], at - far_base, size), 0), (into(near_bufs[0], at + near_shift, size), 0)])
    after_first_columns(w_ref, far_bufs)
    far_rows = far * size - HALO
    far_at = pl.multiple_of(PAD + HALO * upper, 8)
    far_to = pl.multiple_of((strip - far_rows) * upper, 8)
    far_copies = put_rows(far_bufs[0], far_at, far_rows, out.at[0], far_to, out_sem.at[1])
    for copy in far_copies:
        copy.start()
    squares = square_rows(far_bufs[0], far_at, far_rows)

    fourth(CHUNKS - 2)
    finish(CHUNKS - 2, [(into(near_bufs[0], rows(CHUNKS - 2).start + near_shift, size), 0)])
    fourth(CHUNKS - 1)
    fourth(CHUNKS)
    near_last = into(near_bufs[0], rows(CHUNKS - 1).start + near_shift, size)
    finish(CHUNKS - 1, [(near_last, 0), (into(near_bufs[0], near_halo, HALO), size)], halo_of(top))
    after_first_columns(w_ref, near_bufs)
    near_rows = strip - far_rows
    near_to = pl.multiple_of(far_rows * (1 - upper), 8)
    near_copies = put_rows(near_bufs[0], PAD + HALO, near_rows, out.at[0], near_to, out_sem.at[2])
    for copy in near_copies:
        copy.start()
    squares = squares + square_rows(near_bufs[0], PAD + HALO, near_rows)
    copies = copies + far_copies + near_copies
    energy0 = band_energy(squares, jnp.where(odd, 2, 3))
    total = energy0 + energy1 + energy2 + energy3

    def tell(stage, k):
        slot, members = groups[stage]
        return pltpu.make_async_remote_copy(
            src_ref=shared.at[stage, slot],
            dst_ref=shared.at[stage, slot],
            send_sem=sum_send.at[stage, k],
            recv_sem=sum_recv.at[stage, slot],
            device_id=members[k],
            device_id_type=pl.DeviceIdType.MESH,
        )

    def heard(stage, k):
        return pltpu.make_async_remote_copy(
            src_ref=shared.at[stage, k],
            dst_ref=shared.at[stage, k],
            send_sem=sum_send.at[stage, k],
            recv_sem=sum_recv.at[stage, k],
            device_id=groups[stage][1][k],
            device_id_type=pl.DeviceIdType.MESH,
        )

    for stage, (slot, members) in enumerate(groups):
        shared[stage, slot] = total
        for k in range(len(members)):
            pl.when(slot != k)(lambda stage=stage, k=k: tell(stage, k).start())
        for k in range(len(members)):
            pl.when(slot != k)(lambda stage=stage, k=k: heard(stage, k).wait_recv())
        total = functools.reduce(jnp.add, [shared[stage, k] for k in range(len(members))])
    energy_ref[...] = total[:TLEVELS + 1, :3 * SLEVELS + 1] / counts_ref[...]

    for stage, (slot, members) in enumerate(groups):
        for k in range(len(members)):
            pl.when(slot != k)(lambda stage=stage, k=k: tell(stage, k).wait_send())
    for copy in copies:
        copy.wait()
    exchange.wait_send()

    def drain(c):
        send(0, 0, c, g).wait_send()
        send(0, 1, c, g).wait_send()
        send(1, 0, c, s0).wait_send()
        send(1, 1, c, h).wait_send()
        send(2, 0, c, top).wait_send()
        send(2, 1, c, t0).wait_send()

    each(drain)
    drain(CHUNKS)


def copy_kernel(src, energy_in, out, energy_out, stage, small, sems, small_sems):
    parts = stage.shape[0]
    frames, strip = src.shape[:2]
    size = frames * strip // parts

    def ends(k):
        at = pl.ds(k * size % strip, size)
        take = pltpu.make_async_copy(src.at[k * size // strip, at], stage.at[k], sems.at[0, k])
        put = pltpu.make_async_copy(stage.at[k], out.at[k * size // strip, at], sems.at[1, k])
        return take, put

    copies = [ends(k) for k in range(parts)]
    copies.append((
        pltpu.make_async_copy(energy_in, small, small_sems.at[0]),
        pltpu.make_async_copy(small, energy_out, small_sems.at[1]),
    ))
    for take, _ in copies:
        take.start()
    for take, put in copies:
        take.wait()
        put.start()
    for _, put in copies:
        put.wait()


def row_buffers(rows, width):
    return [pltpu.VMEM((width // LANES, rows // k + 3 * PAD, LANES), jnp.float32) for k in (1, 2, 4)]


def shards(footage):
    frames, strip, width = footage.shape
    blocks = jnp.asarray(weight_blocks(width))
    plane = pltpu.VMEM((strip + EXTRA, width), jnp.float32)
    dma = pltpu.SemaphoreType.DMA
    full = jax.ShapeDtypeStruct(footage.shape, jnp.float32)
    hbm = pl.BlockSpec(memory_space=pl.ANY)
    vmem = pl.BlockSpec(memory_space=pltpu.VMEM)
    devices = lax.axis_size("frame")
    size = counts(frames * devices, strip * lax.axis_size("row"), width)
    coeffs, energies = pl.pallas_call(
        time_kernel,
        out_shape=(full, jax.ShapeDtypeStruct(size.shape, jnp.float32)),
        in_specs=[hbm, vmem, vmem, vmem],
        out_specs=(hbm, vmem),
        scratch_shapes=[
            pltpu.VMEM((frames, strip + EXTRA, width), jnp.float32),
            pltpu.VMEM((3, 2, strip + EXTRA, width), jnp.float32),
            *[plane] * 8,
            pltpu.VMEM((frames, HALO, width), jnp.float32),
            pltpu.VMEM((frames, EXTRA, width), jnp.float32),
            pltpu.VMEM((2, 4 * Y_CHIPS, 8, LANES), jnp.float32),
            pltpu.VMEM((SLEVELS, 2, 3, 4 * LANES, 2 * LANES), jnp.bfloat16),
            *row_buffers(strip + HALO, width),
            *row_buffers((CHUNKS - 2) * (strip // CHUNKS), width),
            *row_buffers(3 * (strip // CHUNKS) + HALO, width),
            dma((4,)),
            dma,
            dma((3, 2, CHUNKS + 1)),
            dma((3, 2, CHUNKS + 1)),
            dma((2,)),
            dma((3, width // LANES)),
            dma((2, 4 * Y_CHIPS)),
            dma((2, 4 * Y_CHIPS)),
        ],
        compiler_params=pltpu.CompilerParams(
            collective_id=0, has_side_effects=True, vmem_limit_bytes=60 * 2**20
        ),
        name="time",
    )(footage, blocks, jnp.asarray(summaries()), jnp.asarray(size, jnp.float32))
    parts = 16
    return pl.pallas_call(
        copy_kernel,
        out_shape=(full, jax.ShapeDtypeStruct(size.shape, jnp.float32)),
        in_specs=[hbm, hbm],
        out_specs=(hbm, hbm),
        scratch_shapes=[
            pltpu.VMEM((parts, frames * strip // parts, width), jnp.float32),
            pltpu.VMEM(size.shape, jnp.float32),
            dma((2, parts)),
            dma((2,)),
        ],
        compiler_params=pltpu.CompilerParams(vmem_limit_bytes=60 * 2**20),
        name="copy_out",
    )(coeffs, energies)


def solution(mesh):
    return jax.shard_map(
        shards,
        mesh=mesh,
        in_specs=(P("frame", "row", None),),
        out_specs=(P("frame", "row", None), P()),
        check_vma=False,
    )
```
